256 devices in a mesh: dp: 8 (over y, core), expert: 32 (over x, z).
Axes of the slice: x: 4, y: 4, z: 8, core: 2. Of those that a mesh axis runs over, the one named last changes fastest.
Arguments:
- tokens: bfloat16 [4096, 4096], P(('dp', 'expert')), may hold values from -6 to 6
- expert_ids: int32 [4096, 2], P(('dp', 'expert')), may hold values from 0 to 7, all different within a row; in each aligned block of 16 rows (0 to 15, 16 to 31, ...) at most 6 rows name the same one
- gate_quota: int32 [4096, 2], P(('dp', 'expert')), may hold values from 1 to 32767
- w_gate: bfloat16 [32, 4096, 2048], P('expert', None, 'dp'), may hold values from -0.09375 to 0.09375
- w_up: bfloat16 [32, 4096, 2048], P('expert', None, 'dp'), may hold values from -0.09375 to 0.09375
- w_down: bfloat16 [32, 2048, 4096], P('expert', 'dp'), may hold values from -0.0625 to 0.0625
Outputs:
- mixed_out: bfloat16 [4096, 4096], P(('dp', 'expert'))
The draws below stay inside these ranges and needn't reach their ends.
Inputs may be any that keep to these rules, and one draw needn't show every extreme that they name: `expert_ids`: each row names 2 different experts; among the rows of one device no expert is named more than 6 times.
All inputs are finite; a program needn't handle non-finite values.
Results may differ from the reference program's by a relative error of at most 0.015.
Values may be sent and summed in bfloat16 or wider, within the bound.
A program may use at most 128 MiB of HBM per device.

```python
import math
import jax
import jax.numpy as jnp
import numpy as np
from jax import lax

D = 4096
FF = 8192
EXPERTS = 8
TOP = 2
TOK_DEV = 16
CAP = 6
GROUP = 4
TOKENS = 4096
N_DP = 8
N_EXPERT = 32


def set_ends(array, stream_key, least, largest):
    spot = [jax.random.randint(jax.random.fold_in(stream_key, axis), (), 0, length) for axis, length in enumerate(array.shape)]
    widest = array.shape.index(max(array.shape))
    next_to = spot[:widest] + [(spot[widest] + 1) % array.shape[widest]] + spot[widest + 1:]
    return array.at[tuple(spot)].set(least).at[tuple(next_to)].set(largest)


def level_of(own_key, shape, shards, least, largest):
    gain = 1.0
    for axis_at, parts in shards:
        steps = jax.random.uniform(jax.random.fold_in(jax.random.fold_in(own_key, 6), axis_at), (parts,), jnp.float32, least / len(shards), largest / len(shards))
        gain = gain * jnp.repeat(jnp.exp(steps), shape[axis_at] // parts).reshape((-1,) + (1,) * (len(shape) - 1 - axis_at))
    return gain


def assign_block(stream_key, own, number, rows, amount, top, reach, slope):
    order = jax.random.permutation(stream_key, amount)
    heavy_load, common = load_shares(amount, rows * top, reach, slope, True), load_shares(amount, rows * top, reach, slope, False)
    places = jnp.arange(amount)

    def named(tallies, offset_by):
        used = int((tallies > 0).sum())
        fixed = max(1, used // 4)
        moved = fixed + (places - fixed + offset_by * (used - fixed)) % max(1, amount - fixed)
        return jnp.zeros((amount,), jnp.int32).at[order[jnp.where(places < fixed, places, moved)]].set(jnp.asarray(tallies, jnp.int32))

    tallies = jnp.where(number % 4 == 0, named(heavy_load, number // 4), named(common, number - number // 4 - 1))
    mixed = jax.random.permutation(jax.random.fold_in(own, 3), amount)
    giver, sink = mixed[0:amount // 2 * 2:2], mixed[1:amount // 2 * 2:2]
    room = jnp.minimum(tallies[giver] - 1, reach - tallies[sink]) // 2
    room = jnp.where((giver == order[0]) | (sink == order[0]) | (tallies[sink] == 0), 0, jnp.maximum(room, 0))
    moved = jax.random.randint(jax.random.fold_in(own, 4), (amount // 2,), 0, 1 << 20) % (room + 1)
    tallies = tallies.at[giver].add(-moved).at[sink].add(moved)
    labels = jnp.searchsorted(jnp.cumsum(tallies), jnp.arange(rows * top), side="right").astype(jnp.int32)
    table = labels.reshape(top, rows).T
    table = table[jax.random.permutation(jax.random.fold_in(own, 1), rows)]
    offset_by = jax.random.randint(jax.random.fold_in(own, 2), (rows, 1), 0, top)
    return jnp.take_along_axis(table, (jnp.arange(top)[None, :] + offset_by) % top, axis=1)


def load_shares(amount, total, bound, slope, full):
    weights = [(1 << 20) // math.isqrt(standing ** slope) + 1 for standing in range(1, amount + 1)]
    largest = bound if full else min(bound, max(-(-total // amount), total * weights[0] // sum(weights)))
    least = 1 if total - largest >= amount - 1 else 0
    holding, spare = [largest] + [least] * (amount - 1), total - largest - least * (amount - 1)
    while spare > 0:
        movable = [i for i in range(1, amount) if holding[i] < largest] or [i for i in range(1, amount) if holding[i] < bound]
        whole, budget = sum([weights[i] for i in movable]), spare
        for i in movable:
            addition = min(bound - holding[i], max(1, budget * weights[i] // whole), spare)
            holding[i] = holding[i] + addition
            spare = spare - addition
    return np.array(holding)


def scatter_about(own_key, extent, deviation, bound, shards=(), kind=jnp.bfloat16):
    gain = level_of(own_key, extent, shards, -0.22, 0.18) if shards else 1.0
    entries = jax.random.normal(own_key, extent, jnp.float32) * deviation * gain
    return jnp.minimum(jnp.maximum(entries, -bound), bound).astype(kind)


def setup_inputs(seed: int = 0) -> dict:
    key_of = jax.random.split(jax.random.key(seed), 7)
    tokens = scatter_about(key_of[0], (TOKENS, D), 1.0, 6.0, ((0, 256),))
    expert_ids_keys = jax.random.split(jax.random.fold_in(key_of[1], 1), TOKENS // TOK_DEV)
    expert_ids_turns = jax.random.permutation(jax.random.fold_in(key_of[1], 3), TOKENS // TOK_DEV)
    expert_ids = jax.vmap(lambda own, number: assign_block(jax.random.fold_in(key_of[1], 2), own, number, TOK_DEV, EXPERTS, TOP, CAP, 2))(expert_ids_keys, expert_ids_turns).reshape((TOKENS, TOP))
    gate_quota = set_ends(jax.random.randint(key_of[2], (TOKENS, TOP), 1, 32768), jax.random.fold_in(key_of[2], 1), 1, 32767).astype(jnp.int32)
    w_gate = scatter_about(key_of[3], (EXPERTS * GROUP, D, FF // GROUP), D ** -0.5, 0.09375, ((0, 32), (2, 8)))
    w_up = scatter_about(key_of[4], (EXPERTS * GROUP, D, FF // GROUP), D ** -0.5, 0.09375, ((0, 32), (2, 8)))
    w_down = scatter_about(key_of[5], (EXPERTS * GROUP, FF // GROUP, D), FF ** -0.5, 0.0625, ((0, 32), (1, 8)))
    return {"tokens": tokens, "expert_ids": expert_ids, "gate_quota": gate_quota, "w_gate": w_gate, "w_up": w_up, "w_down": w_down}


def reference(tokens, expert_ids, gate_quota, w_gate, w_up, w_down):
    col_count = FF // GROUP
    block_count = GROUP * N_DP
    block_width = FF // block_count
    gate_all = w_gate.reshape(EXPERTS, GROUP, D, col_count).transpose(0, 2, 1, 3).reshape(EXPERTS, D, FF)
    up_all = w_up.reshape(EXPERTS, GROUP, D, col_count).transpose(0, 2, 1, 3).reshape(EXPERTS, D, FF)
    down_all = w_down.reshape(EXPERTS, FF, D)
    flat_ids = expert_ids.reshape(-1)
    most_rows = CAP * N_DP * N_EXPERT
    per_assign = jnp.zeros((TOKENS * TOP, D), jnp.float32)

    def add_block(running, operands):
        term = jnp.dot(operands[0], operands[1], preferred_element_type=jnp.float32).astype(jnp.bfloat16)
        term = lax.optimization_barrier(term)
        return running + term.astype(jnp.float32), None

    for expert in range(EXPERTS):
        picked = flat_ids == expert
        chosen = jnp.nonzero(picked, size=most_rows, fill_value=0)[0].astype(jnp.int32)
        is_valid = (jnp.arange(most_rows, dtype=jnp.int32) < jnp.sum(picked.astype(jnp.int32))).astype(jnp.float32)
        expert_rows = tokens[chosen // TOP]
        gate_act = jnp.dot(expert_rows, gate_all[expert], preferred_element_type=jnp.float32)
        up_act = jnp.dot(expert_rows, up_all[expert], preferred_element_type=jnp.float32)
        hidden = (jax.nn.silu(gate_act) * up_act).astype(jnp.bfloat16)
        hidden_blocks = hidden.reshape(most_rows, block_count, block_width).transpose(1, 0, 2)
        down_blocks = down_all[expert].reshape(block_count, block_width, D)
        out_rows, _ = lax.scan(add_block, jnp.zeros((most_rows, D), jnp.float32), (hidden_blocks, down_blocks))
        per_assign = per_assign.at[chosen].add(out_rows * is_valid[:, None])
    quota = gate_quota.astype(jnp.float32)
    shares = quota / jnp.sum(quota, axis=1, keepdims=True)
    mixed_out = jnp.sum(per_assign.reshape(TOKENS, TOP, D) * shares[:, :, None], axis=1)
    return mixed_out.astype(jnp.bfloat16)
```

```python
import jax
import jax.numpy as jnp
from jax import lax
from jax.experimental import pallas as pl
from jax.experimental.pallas import tpu as pltpu
from jax.sharding import PartitionSpec as P

MESH = pl.DeviceIdType.MESH
EXPERTS = 8
TOP = 2
CAP = 6
NX = 4
NZ = 8
NY = 4
HALVES = EXPERTS // NX
GROUP = NZ // HALVES
SPLIT = 8
NCHUNK = NX
F32 = jnp.float32
BF16 = jnp.bfloat16


def moe_kernel(
    tok_ref, pick_ref, mix_ref, perm_ref, wg_hbm, wu_hbm, wd_hbm, out_ref,
    packed, arr, xall, wg, wu, wd, hid, part, fromcore, ringa, ringb, lasta, lastb, outgo, ret,
    w_sem, dsend, drecv, gsend, grecv, rsend, rrecv, bsend, brecv,
):
    feature = tok_ref.shape[1]
    piece = feature // SPLIT
    half = feature // 2
    rows = NZ * CAP
    dp = lax.axis_index("dp")
    ex = lax.axis_index("expert")
    core = lax.rem(dp, 2)
    y = dp // 2
    xx = ex // NZ
    zz = lax.rem(ex, NZ)
    n_ex = NX * NZ
    y_up, y_down, y_far = lax.rem(y + 1, NY), lax.rem(y + NY - 1, NY), lax.rem(y + 2, NY)
    up = y_up * 2 + core
    down = y_down * 2 + core
    far = y_far * 2 + core
    other = y * 2 + (1 - core)
    lo = pl.ds(0, half)
    hi = pl.ds(half, half)

    loads = [
        pltpu.make_async_copy(wg_hbm.at[0], wg, w_sem.at[0]),
        pltpu.make_async_copy(wu_hbm.at[0], wu, w_sem.at[1]),
        pltpu.make_async_copy(wd_hbm.at[0], wd, w_sem.at[2]),
    ]
    for load in loads:
        load.start()

    barrier = pltpu.get_barrier_semaphore()

    def greet(i, carry):
        pl.semaphore_signal(
            barrier, inc=1, device_id={"expert": lax.rem(ex + i, n_ex)}, device_id_type=MESH
        )
        return carry

    lax.fori_loop(1, n_ex, greet, 0)
    for peer in (up, down, other):
        pl.semaphore_signal(barrier, inc=1, device_id={"dp": peer}, device_id_type=MESH)

    stacked = jnp.concatenate(
        [tok_ref[:, o * piece : (o + 1) * piece] for o in range(SPLIT)], axis=0
    )
    chosen = jnp.dot(pick_ref[...], stacked, preferred_element_type=F32).astype(BF16)
    packed[...] = chosen.reshape(packed.shape)
    arr[0, pl.ds(zz, 1)] = packed[0, pl.ds(zz // GROUP, 1)]

    pl.semaphore_wait(barrier, n_ex - 1 + 3)

    def to_expert(k, dz):
        z_to = lax.rem(zz + dz, NZ)
        x_to = lax.rem(xx + k, NX)
        return pltpu.make_async_remote_copy(
            packed.at[k, z_to // GROUP], arr.at[k, zz], dsend.at[k, dz], drecv.at[k, zz],
            device_id={"expert": x_to * NZ + z_to}, device_id_type=MESH,
        )

    def expert_arrival(k, z_from):
        return pltpu.make_async_remote_copy(
            packed.at[k, 0], arr.at[k, z_from], dsend.at[k, 0], drecv.at[k, z_from],
            device_id={"expert": ex}, device_id_type=MESH,
        )

    def to_dp(src, dst, send, recv, peer):
        return pltpu.make_async_remote_copy(
            src, dst, send, recv, device_id={"dp": peer}, device_id_type=MESH
        )

    def g_copy(k, n):
        send, recv = gsend.at[k, n], grecv.at[k, n]
        block, cols, peer = [
            (dp, None, up), (dp, None, down), (dp, None, other),
            (down, lo, up), (up, hi, down),
            (down, None, other), (up, None, other), (far, None, other),
        ][n]
        view = xall.at[k, block] if cols is None else xall.at[k, block, :, cols]
        return to_dp(view, view, send, recv, peer)

    def r_copy(k, n):
        send, recv = rsend.at[k, n], rrecv.at[k, n]
        if n < 4:
            place = [y_far, y_up, y_down, y][n]
            return to_dp(
                part.at[k, place * 2 + (1 - core)], fromcore.at[k, place], send, recv, other
            )
        src, cols, dst, peer = [
            (far, lo, ringa.at[k], up),
            (far, hi, ringb.at[k], down),
            (up, hi, lasta.at[k, :, hi], up),
            (down, lo, lastb.at[k, :, lo], down),
            (up, lo, lasta.at[k, :, lo], up),
            (down, hi, lastb.at[k, :, hi], down),
        ][n - 4]
        return to_dp(part.at[k, src, :, cols], dst, send, recv, peer)

    def to_owner(k, dz):
        z_to = lax.rem(zz + dz, NZ)
        x_to = lax.rem(xx + NX - k, NX)
        return pltpu.make_async_remote_copy(
            outgo.at[k, z_to], ret.at[k, zz], bsend.at[k, dz], brecv.at[k, zz],
            device_id={"expert": x_to * NZ + z_to}, device_id_type=MESH,
        )

    def owner_arrival(k, z_from):
        return pltpu.make_async_remote_copy(
            outgo.at[k, 0], ret.at[k, z_from], bsend.at[k, 0], brecv.at[k, z_from],
            device_id={"expert": ex}, device_id_type=MESH,
        )

    def send_all(k, carry):
        def one(dz, inner):
            @pl.when((k != 0) | (dz != 0))
            def _():
                to_expert(k, dz).start()

            return inner

        return lax.fori_loop(0, NZ, one, carry)

    lax.fori_loop(0, NCHUNK, send_all, 0)

    def stage_rows(k):
        def one(z_from, inner):
            @pl.when((k != 0) | (z_from != zz))
            def _():
                expert_arrival(k, z_from).wait_recv()

            return inner

        lax.fori_loop(0, NZ, one, 0)
        flat = arr[k].reshape(NZ * CAP * SPLIT, piece)
        sorted_rows = jnp.dot(perm_ref[0], flat, preferred_element_type=F32).astype(BF16)
        for o in range(SPLIT):
            xall[k, dp, :, o * piece : (o + 1) * piece] = sorted_rows[o * rows : (o + 1) * rows]
        for n in range(3):
            g_copy(k, n).start()

    def stage_forward(k):
        g_copy(k, 0).wait_recv()
        g_copy(k, 3).start()
        g_copy(k, 5).start()
        g_copy(k, 1).wait_recv()
        g_copy(k, 4).start()
        g_copy(k, 6).start()

    def stage_far(k):
        g_copy(k, 3).wait_recv()
        g_copy(k, 4).wait_recv()
        g_copy(k, 7).start()

    def stage_compute(k):
        for n in (2, 5, 6, 7):
            g_copy(k, n).wait_recv()

        @pl.when(k == 0)
        def _():
            for load in loads:
                load.wait()

        for m in range(2):
            x_in = xall[k, m * NY : (m + 1) * NY].reshape(NY * rows, feature)
            gate = jnp.dot(x_in, wg[...], preferred_element_type=F32)
            up_act = jnp.dot(x_in, wu[...], preferred_element_type=F32)
            hid[m * NY * rows : (m + 1) * NY * rows] = (
                gate * (1.0 / (1.0 + jnp.exp(-gate))) * up_act
            ).astype(BF16)

        def down_block(n, carry):
            cols = pl.ds(pl.multiple_of(n * piece, piece), piece)
            got = jnp.dot(hid[...], wd[:, cols], preferred_element_type=F32).astype(BF16)
            part[k, :, :, cols] = got.reshape(2 * NY, rows, piece)
            return carry

        lax.fori_loop(0, SPLIT, down_block, 0)
        for n in range(4):
            r_copy(k, n).start()

    def join(k, place, cols):
        mine = place * 2 + core
        total = part[k, mine, :, cols].astype(F32) + fromcore[k, place, :, cols].astype(F32)
        part[k, mine, :, cols] = total.astype(BF16)

    def stage_ring(k):
        r_copy(k, 0).wait_recv()
        join(k, y_far, pl.ds(0, feature))
        r_copy(k, 4).start()
        r_copy(k, 5).start()
        r_copy(k, 1).wait_recv()
        join(k, y_up, pl.ds(0, feature))
        r_copy(k, 6).start()
        r_copy(k, 2).wait_recv()
        join(k, y_down, pl.ds(0, feature))
        r_copy(k, 7).start()

    def stage_last(k):
        r_copy(k, 4).wait_recv()
        part[k, up, :, lo] = (part[k, up, :, lo].astype(F32) + ringa[k].astype(F32)).astype(BF16)
        r_copy(k, 8).start()
        r_copy(k, 5).wait_recv()
        part[k, down, :, hi] = (
            part[k, down, :, hi].astype(F32) + ringb[k].astype(F32)
        ).astype(BF16)
        r_copy(k, 9).start()

    def stage_back(k):
        r_copy(k, 3).wait_recv()
        for n in (6, 7, 8, 9):
            r_copy(k, n).wait_recv()
        pieces = []
        for o in range(SPLIT):
            cols = slice(o * piece, (o + 1) * piece)
            total = (
                part[k, dp, :, cols].astype(F32)
                + fromcore[k, y, :, cols].astype(F32)
                + lasta[k, :, cols].astype(F32)
                + lastb[k, :, cols].astype(F32)
            )
            pieces.append(total.astype(BF16))
        block = jnp.concatenate(pieces, axis=0)
        sorted_rows = jnp.dot(perm_ref[1], block, preferred_element_type=F32).astype(BF16)
        outgo[k] = sorted_rows.reshape(NZ, CAP * SPLIT, piece)

        def one(dz, inner):
            @pl.when((k != 0) | (dz != 0))
            def _():
                to_owner(k, dz).start()

            return inner

        lax.fori_loop(0, NZ, one, 0)

        @pl.when(k == 0)
        def _():
            ret[0, pl.ds(zz, 1)] = outgo[0, pl.ds(zz, 1)]

    def step(i, carry):
        j = i - 1
        for stage, lag in (
            (stage_forward, 0), (stage_rows, -1), (stage_ring, 1), (stage_back, 2),
            (stage_far, 0), (stage_compute, 0), (stage_last, 1),
        ):
            k = j - lag

            @pl.when((k >= 0) & (k < NCHUNK))
            def _(stage=stage, k=k):
                stage(k)

        return carry

    lax.fori_loop(0, NCHUNK + 3, step, 0)

    def drain(k, carry):
        def one(z, inner):
            @pl.when((k != 0) | (z != zz))
            def _():
                owner_arrival(k, z).wait_recv()

            @pl.when((k != 0) | (z != 0))
            def _():
                to_expert(k, z).wait_send()
                to_owner(k, z).wait_send()

            return inner

        lax.fori_loop(0, NZ, one, 0)
        for n in range(8):
            g_copy(k, n).wait_send()
        for n in range(10):
            r_copy(k, n).wait_send()
        return carry

    lax.fori_loop(0, NCHUNK, drain, 0)

    sums = []
    for k in range(NX):
        for h in range(HALVES):
            total = ret[k, h * GROUP].astype(F32)
            for g in range(1, GROUP):
                total = total + ret[k, h * GROUP + g].astype(F32)
            sums.append(total)
    mixed = jnp.dot(
        mix_ref[...], jnp.concatenate(sums, axis=0),
        preferred_element_type=F32, precision=lax.Precision.HIGHEST,
    ).astype(BF16)
    tok = tok_ref.shape[0]
    for o in range(SPLIT):
        out_ref[:, o * piece : (o + 1) * piece] = mixed[o * tok : (o + 1) * tok]


def on_device(tokens, expert_ids, gate_quota, w_gate, w_up, w_down):
    tok_rows, feature = tokens.shape
    width = w_gate.shape[2]
    piece = feature // SPLIT
    rows = NZ * CAP
    slots = EXPERTS * CAP
    flat_ids = expert_ids.reshape(-1)
    chosen_mask = (flat_ids[:, None] == jnp.arange(EXPERTS, dtype=jnp.int32)[None, :]).astype(
        jnp.int32
    )
    earlier = jnp.cumsum(chosen_mask, axis=0) - chosen_mask
    position = jnp.sum(earlier * chosen_mask, axis=1)
    xx = lax.axis_index("expert") // NZ
    ahead = (flat_ids // HALVES + NX - xx) % NX
    slot = ((ahead * HALVES + flat_ids % HALVES) * CAP + position).reshape(tok_rows, TOP)
    quota = gate_quota.astype(F32)
    shares = quota / jnp.sum(quota, axis=1, keepdims=True)
    match = slot[:, :, None] == jnp.arange(slots, dtype=jnp.int32)
    picked = jnp.any(match, axis=1)
    weight = jnp.sum(jnp.where(match, shares[:, :, None], 0.0), axis=1)
    same = jnp.eye(SPLIT, dtype=bool)
    pick = jnp.where(same[None, :, :, None], picked.T[:, None, None, :], False).astype(BF16)
    pick = pick.reshape(slots * SPLIT, SPLIT * tok_rows)
    mix = jnp.where(same[:, None, None, :], weight[None, :, :, None], 0.0)
    mix = mix.reshape(SPLIT * tok_rows, slots * SPLIT)
    index = jnp.arange(rows * SPLIT, dtype=jnp.int32)
    wanted = (index % rows) * SPLIT + index // rows
    perm = (wanted[:, None] == index[None, :]).astype(BF16)
    perms = jnp.stack([perm, perm.T])

    whole = pl.BlockSpec(memory_space=pltpu.VMEM)
    anywhere = pl.BlockSpec(memory_space=pl.ANY)
    dma = pltpu.SemaphoreType.DMA
    return pl.pallas_call(
        moe_kernel,
        out_shape=jax.ShapeDtypeStruct((tok_rows, feature), BF16),
        in_specs=[whole, whole, whole, whole, anywhere, anywhere, anywhere],
        out_specs=whole,
        scratch_shapes=[
            pltpu.VMEM((NX, HALVES, CAP * SPLIT, piece), BF16),
            pltpu.VMEM((NX, NZ, CAP * SPLIT, piece), BF16),
            pltpu.VMEM((NX, 2 * NY, rows, feature), BF16),
            pltpu.VMEM((feature, width), BF16),
            pltpu.VMEM((feature, width), BF16),
            pltpu.VMEM((width, feature), BF16),
            pltpu.VMEM((2 * NY * rows, width), BF16),
            pltpu.VMEM((NX, 2 * NY, rows, feature), BF16),
            pltpu.VMEM((NX, NY, rows, feature), BF16),
            pltpu.VMEM((NX, rows, feature // 2), BF16),
            pltpu.VMEM((NX, rows, feature // 2), BF16),
            pltpu.VMEM((NX, rows, feature), BF16),
            pltpu.VMEM((NX, rows, feature), BF16),
            pltpu.VMEM((NX, NZ, CAP * SPLIT, piece), BF16),
            pltpu.VMEM((NX, NZ, CAP * SPLIT, piece), BF16),
            dma((3,)),
            dma((NX, NZ)),
            dma((NX, NZ)),
            dma((NX, 8)),
            dma((NX, 8)),
            dma((NX, 10)),
            dma((NX, 10)),
            dma((NX, NZ)),
            dma((NX, NZ)),
        ],
        compiler_params=pltpu.CompilerParams(
            collective_id=0, has_side_effects=True, vmem_limit_bytes=64 * 1024 * 1024 - 65536
        ),
        name="moe",
    )(tokens, pick, mix, perms, w_gate, w_up, w_down)


def solution(mesh):
    return jax.shard_map(
        on_device,
        mesh=mesh,
        in_specs=(
            P(("dp", "expert"), None),
            P(("dp", "expert"), None),
            P(("dp", "expert"), None),
            P("expert", None, "dp"),
            P("expert", None, "dp"),
            P("expert", "dp", None),
        ),
        out_specs=P(("dp", "expert"), None),
        check_vma=False,
    )
```

```python
import jax
import jax.numpy as jnp
from jax import lax
from jax.experimental import pallas as pl
from jax.experimental.pallas import tpu as pltpu
from jax.sharding import PartitionSpec as P

MESH = pl.DeviceIdType.MESH
EXPERTS = 8
TOP = 2
CAP = 6
NX = 4
NZ = 8
NY = 4
HALVES = EXPERTS // NX
GROUP = NZ // HALVES
SPLIT = 8
NCHUNK = NX
F32 = jnp.float32
BF16 = jnp.bfloat16

STAGES = (
    ("forward_0", 0), ("rows_0", -1), ("forward_1", 0), ("rows_1", -1),
    ("ring_0", 1), ("ring_1", 1), ("far_0", 0), ("far_1", 0), ("compute", 0),
    ("back_0", 2), ("back_1", 2), ("last_0", 1), ("last_1", 1),
)


def moe_kernel(
    tok_hbm, ids_hbm, quota_hbm, wg_hbm, wu_hbm, wd_hbm, out_ref,
    tok_ref, ids_ref, quota_ref, packed, arr, xall, wg, wu, wd, hid, part, fromcore, ringa, ringb, lasta, lastb, outgo, ret,
    perm, mix, w_sem, dsend, drecv, gsend, grecv, rsend, rrecv, bsend, brecv,
):
    tok, feature = tok_ref.shape
    half = feature // 2
    quarter = feature // 4
    piece = half // SPLIT
    rows = NZ * CAP
    slots = EXPERTS * CAP
    dp = lax.axis_index("dp")
    ex = lax.axis_index("expert")
    core = lax.rem(dp, 2)
    y = dp // 2
    xx = ex // NZ
    zz = lax.rem(ex, NZ)
    n_ex = NX * NZ
    y_up, y_down, y_far = lax.rem(y + 1, NY), lax.rem(y + NY - 1, NY), lax.rem(y + 2, NY)
    up = y_up * 2 + core
    down = y_down * 2 + core
    far = y_far * 2 + core
    other = y * 2 + (1 - core)

    def both(c):
        return pl.ds(c * half, half)

    def lo(c):
        return pl.ds(c * half, quarter)

    def hi(c):
        return pl.ds(c * half + quarter, quarter)

    barrier = pltpu.get_barrier_semaphore()

    def greet(i, carry):
        pl.semaphore_signal(
            barrier, inc=1, device_id={"expert": lax.rem(ex + i, n_ex)}, device_id_type=MESH
        )
        return carry

    lax.fori_loop(1, n_ex, greet, 0)
    for peer in (up, down, other):
        pl.semaphore_signal(barrier, inc=1, device_id={"dp": peer}, device_id_type=MESH)

    first_loads = [
        pltpu.make_async_copy(ids_hbm, ids_ref, w_sem.at[3]),
        pltpu.make_async_copy(quota_hbm, quota_ref, w_sem.at[4]),
        pltpu.make_async_copy(tok_hbm, tok_ref, w_sem.at[5]),
    ]
    for load in first_loads:
        load.start()
    loads = [
        pltpu.make_async_copy(wg_hbm.at[0], wg, w_sem.at[0]),
        pltpu.make_async_copy(wu_hbm.at[0], wu, w_sem.at[1]),
        pltpu.make_async_copy(wd_hbm.at[0], wd, w_sem.at[2]),
    ]
    for load in loads:
        load.start()

    p_row = lax.broadcasted_iota(jnp.int32, (rows * SPLIT, rows * SPLIT), 0)
    p_col = lax.broadcasted_iota(jnp.int32, (rows * SPLIT, rows * SPLIT), 1)
    perm[0] = jnp.where(p_row == (p_col & (SPLIT - 1)) * rows + (p_col >> 3), 1.0, 0.0).astype(BF16)

    for load in first_loads:
        load.wait()

    lanes = SPLIT * tok
    t_row = lax.broadcasted_iota(jnp.int32, (tok, lanes), 0)
    t_col = lax.broadcasted_iota(jnp.int32, (tok, lanes), 1) & (tok - 1)
    eye = lax.broadcasted_iota(jnp.int32, (tok, tok), 0) == lax.broadcasted_iota(
        jnp.int32, (tok, tok), 1
    )

    def spread(values):
        grid = jnp.where(eye, jnp.broadcast_to(values, (tok, tok)), 0)
        return jnp.broadcast_to(jnp.sum(grid, axis=1, keepdims=True), (tok, lanes))

    ids = [spread(ids_ref[k : k + 1, :]) for k in range(TOP)]
    quota = [spread(quota_ref[k : k + 1, :].astype(F32)) for k in range(TOP)]
    place_of, share_of = [], []
    lane_quota = [
        jnp.sum(jnp.where(t_row == t_col, q, 0.0), axis=0, keepdims=True) for q in quota
    ]
    whole_quota = lane_quota[0] + lane_quota[1]
    for k in range(TOP):
        mine = jnp.sum(jnp.where(t_row == t_col, ids[k], 0), axis=0, keepdims=True)
        before = jnp.zeros((tok, lanes), jnp.int32)
        for other_k in range(TOP):
            before = before + jnp.where((ids[other_k] == mine) & (t_row < t_col), 1, 0)
        position = jnp.sum(before, axis=0, keepdims=True)
        ahead = ((mine // HALVES) + NX - xx) & (NX - 1)
        place_of.append((ahead * HALVES + (mine & (HALVES - 1))) * CAP + position)
        share_of.append(lane_quota[k] / whole_quota)
    s_row = lax.broadcasted_iota(jnp.int32, (slots * SPLIT, lanes), 0)
    s_col = lax.broadcasted_iota(jnp.int32, (slots * SPLIT, lanes), 1)
    same_piece = (s_row & (SPLIT - 1)) == (s_col >> (tok.bit_length() - 1))
    hits = [same_piece & ((s_row >> 3) == place_of[k]) for k in range(TOP)]
    pick = (jnp.where(hits[0], 1.0, 0.0) + jnp.where(hits[1], 1.0, 0.0)).astype(BF16)

    for c in range(2):
        stacked = jnp.concatenate(
            [
                tok_ref[:, c * half + o * piece : c * half + (o + 1) * piece]
                for o in range(SPLIT)
            ],
            axis=0,
        )
        chosen = jnp.dot(pick, stacked, preferred_element_type=F32).astype(BF16)
        packed[c] = chosen.reshape(NX, HALVES, CAP * SPLIT, piece)
        arr[c, 0, pl.ds(zz, 1)] = packed[c, 0, pl.ds(zz // GROUP, 1)]

    pl.semaphore_wait(barrier, n_ex - 1 + 3)

    def to_expert(k, c, dz):
        z_to = lax.rem(zz + dz, NZ)
        x_to = lax.rem(xx + k, NX)
        return pltpu.make_async_remote_copy(
            packed.at[c, k, z_to // GROUP], arr.at[c, k, zz],
            dsend.at[c, k, dz], drecv.at[c, k, zz],
            device_id={"expert": x_to * NZ + z_to}, device_id_type=MESH,
        )

    def expert_arrival(k, c, z_from):
        return pltpu.make_async_remote_copy(
            packed.at[c, k, 0], arr.at[c, k, z_from], dsend.at[c, k, 0], drecv.at[c, k, z_from],
            device_id={"expert": ex}, device_id_type=MESH,
        )

    def to_dp(src, dst, send, recv, peer):
        return pltpu.make_async_remote_copy(
            src, dst, send, recv, device_id={"dp": peer}, device_id_type=MESH
        )

    def g_copy(k, c, n):
        block, cols, peer = [
            (dp, both(c), up), (dp, both(c), down), (dp, both(c), other),
            (down, lo(c), up), (up, hi(c), down),
            (down, both(c), other), (up, both(c), other), (far, both(c), other),
        ][n]
        view = xall.at[k, block, :, cols]
        return to_dp(view, view, gsend.at[c, k, n], grecv.at[c, k, n], peer)

    def r_copy(k, c, n):
        send, recv = rsend.at[c, k, n], rrecv.at[c, k, n]
        if n < 4:
            place = [y_far, y_up, y_down, y][n]
            return to_dp(
                part.at[k, place * 2 + (1 - core), :, both(c)],
                fromcore.at[k, place, :, both(c)], send, recv, other,
            )
        src, cols, dst, peer = [
            (far, lo(c), ringa.at[c, k], up),
            (far, hi(c), ringb.at[c, k], down),
            (up, hi(c), lasta.at[k, :, hi(c)], up),
            (down, lo(c), lastb.at[k, :, lo(c)], down),
            (up, lo(c), lasta.at[k, :, lo(c)], up),
            (down, hi(c), lastb.at[k, :, hi(c)], down),
        ][n - 4]
        return to_dp(part.at[k, src, :, cols], dst, send, recv, peer)

    def to_owner(k, c, dz):
        z_to = lax.rem(zz + dz, NZ)
        x_to = lax.rem(xx + NX - k, NX)
        return pltpu.make_async_remote_copy(
            outgo.at[c, k, z_to], ret.at[c, k, zz], bsend.at[c, k, dz], brecv.at[c, k, zz],
            device_id={"expert": x_to * NZ + z_to}, device_id_type=MESH,
        )

    def owner_arrival(k, c, z_from):
        return pltpu.make_async_remote_copy(
            outgo.at[c, k, 0], ret.at[c, k, z_from], bsend.at[c, k, 0], brecv.at[c, k, z_from],
            device_id={"expert": ex}, device_id_type=MESH,
        )

    def each_z(k, action):
        def one(z, inner):
            action(z)
            return inner

        lax.fori_loop(0, NZ, one, 0)

    def send_all(k, carry):
        for c in range(2):
            def one(dz):
                @pl.when((k != 0) | (dz != 0))
                def _():
                    to_expert(k, c, dz).start()

            each_z(k, one)
        return carry

    lax.fori_loop(0, NCHUNK, send_all, 0)

    perm[1] = jnp.where(p_col == (p_row & (SPLIT - 1)) * rows + (p_row >> 3), 1.0, 0.0).astype(BF16)
    mix_t = jnp.where(hits[0], share_of[0], 0.0) + jnp.where(hits[1], share_of[1], 0.0)
    mix[...] = mix_t.T

    def stage_rows(k, c):
        def one(z_from):
            @pl.when((k != 0) | (z_from != zz))
            def _():
                expert_arrival(k, c, z_from).wait_recv()

        each_z(k, one)
        flat = arr[c, k].reshape(NZ * CAP * SPLIT, piece)
        sorted_rows = jnp.dot(perm[0], flat, preferred_element_type=F32).astype(BF16)
        for o in range(SPLIT):
            xall[k, dp, :, c * half + o * piece : c * half + (o + 1) * piece] = sorted_rows[
                o * rows : (o + 1) * rows
            ]
        for n in range(3):
            g_copy(k, c, n).start()

    def stage_forward(k, c):
        g_copy(k, c, 0).wait_recv()
        g_copy(k, c, 3).start()
        g_copy(k, c, 5).start()
        g_copy(k, c, 1).wait_recv()
        g_copy(k, c, 4).start()
        g_copy(k, c, 6).start()

    def stage_far(k, c):
        g_copy(k, c, 3).wait_recv()
        g_copy(k, c, 4).wait_recv()
        g_copy(k, c, 7).start()

    def stage_compute(k):
        for c in range(2):
            for n in (2, 5, 6, 7):
                g_copy(k, c, n).wait_recv()

        @pl.when(k == 0)
        def _():
            for load in loads:
                load.wait()

        for m in range(2):
            x_in = xall[k, m * NY : (m + 1) * NY].reshape(NY * rows, feature)
            gate = jnp.dot(x_in, wg[...], preferred_element_type=F32)
            up_act = jnp.dot(x_in, wu[...], preferred_element_type=F32)
            hid[m * NY * rows : (m + 1) * NY * rows] = (
                gate * (1.0 / (1.0 + jnp.exp(-gate))) * up_act
            ).astype(BF16)

        wide = half // 4
        for c in range(2):
            def down_block(n, carry):
                cols = pl.ds(pl.multiple_of(c * half + n * wide, wide), wide)
                got = jnp.dot(hid[...], wd[:, cols], preferred_element_type=F32).astype(BF16)
                part[k, :, :, cols] = got.reshape(2 * NY, rows, wide)
                return carry

            lax.fori_loop(0, 4, down_block, 0)
            for n in range(4):
                r_copy(k, c, n).start()

    def join(k, c, place):
        mine = place * 2 + core
        cols = both(c)
        total = part[k, mine, :, cols].astype(F32) + fromcore[k, place, :, cols].astype(F32)
        part[k, mine, :, cols] = total.astype(BF16)

    def stage_ring(k, c):
        r_copy(k, c, 0).wait_recv()
        join(k, c, y_far)
        r_copy(k, c, 4).start()
        r_copy(k, c, 5).start()
        r_copy(k, c, 1).wait_recv()
        join(k, c, y_up)
        r_copy(k, c, 6).start()
        r_copy(k, c, 2).wait_recv()
        join(k, c, y_down)
        r_copy(k, c, 7).start()

    def stage_last(k, c):
        r_copy(k, c, 4).wait_recv()
        part[k, up, :, lo(c)] = (
            part[k, up, :, lo(c)].astype(F32) + ringa[c, k].astype(F32)
        ).astype(BF16)
        r_copy(k, c, 8).start()
        r_copy(k, c, 5).wait_recv()
        part[k, down, :, hi(c)] = (
            part[k, down, :, hi(c)].astype(F32) + ringb[c, k].astype(F32)
        ).astype(BF16)
        r_copy(k, c, 9).start()

    def stage_back(k, c):
        r_copy(k, c, 3).wait_recv()
        for n in (6, 7, 8, 9):
            r_copy(k, c, n).wait_recv()
        pieces = []
        for o in range(SPLIT):
            cols = slice(c * half + o * piece, c * half + (o + 1) * piece)
            total = (
                part[k, dp, :, cols].astype(F32)
                + fromcore[k, y, :, cols].astype(F32)
                + lasta[k, :, cols].astype(F32)
                + lastb[k, :, cols].astype(F32)
            )
            pieces.append(total.astype(BF16))
        block = jnp.concatenate(pieces, axis=0)
        sorted_rows = jnp.dot(perm[1], block, preferred_element_type=F32).astype(BF16)
        outgo[c, k] = sorted_rows.reshape(NZ, CAP * SPLIT, piece)

        def one(dz):
            @pl.when((k != 0) | (dz != 0))
            def _():
                to_owner(k, c, dz).start()

        each_z(k, one)

        @pl.when(k == 0)
        def _():
            ret[c, 0, pl.ds(zz, 1)] = outgo[c, 0, pl.ds(zz, 1)]

    def step(i, carry):
        j = i - 1
        for stage, lag in STAGES:
            k = j - lag

            @pl.when((k >= 0) & (k < NCHUNK))
            def _(stage=stage, k=k):
                if stage == "compute":
                    stage_compute(k)
                    return
                name, c = stage.split("_")
                todo = {
                    "rows": stage_rows, "forward": stage_forward, "far": stage_far,
                    "ring": stage_ring, "last": stage_last, "back": stage_back,
                }[name]
                todo(k, int(c))

        return carry

    lax.fori_loop(0, NCHUNK + 3, step, 0)

    sums = []
    for c in range(2):
        def arrived(k, carry):
            def one(z):
                @pl.when((k != 0) | (z != zz))
                def _():
                    owner_arrival(k, c, z).wait_recv()

            each_z(k, one)
            return carry

        lax.fori_loop(0, NCHUNK, arrived, 0)
        sums = []
        for k in range(NX):
            for h in range(HALVES):
                total = ret[c, k, h * GROUP].astype(F32)
                for g in range(1, GROUP):
                    total = total + ret[c, k, h * GROUP + g].astype(F32)
                sums.append(total)
        mixed = jnp.dot(
            mix[...], jnp.concatenate(sums, axis=0),
            preferred_element_type=F32, precision=lax.Precision.HIGHEST,
        ).astype(BF16)
        for o in range(SPLIT):
            out_ref[:, c * half + o * piece : c * half + (o + 1) * piece] = mixed[
                o * tok : (o + 1) * tok
            ]

    def drain(k, carry):
        for c in range(2):
            def one(z):
                @pl.when((k != 0) | (z != 0))
                def _():
                    to_expert(k, c, z).wait_send()
                    to_owner(k, c, z).wait_send()

            each_z(k, one)
            for n in range(8):
                g_copy(k, c, n).wait_send()
            for n in range(10):
                r_copy(k, c, n).wait_send()
        return carry

    lax.fori_loop(0, NCHUNK, drain, 0)


def on_device(tokens, expert_ids, gate_quota, w_gate, w_up, w_down):
    tok_rows, feature = tokens.shape
    width = w_gate.shape[2]
    half = feature // 2
    piece = half // SPLIT
    rows = NZ * CAP
    whole = pl.BlockSpec(memory_space=pltpu.VMEM)
    anywhere = pl.BlockSpec(memory_space=pl.ANY)
    dma = pltpu.SemaphoreType.DMA
    return pl.pallas_call(
        moe_kernel,
        out_shape=jax.ShapeDtypeStruct((tok_rows, feature), BF16),
        in_specs=[anywhere] * 6,
        out_specs=whole,
        scratch_shapes=[
            pltpu.VMEM((tok_rows, feature), BF16),
            pltpu.VMEM((TOP, tok_rows), jnp.int32),
            pltpu.VMEM((TOP, tok_rows), jnp.int32),
            pltpu.VMEM((2, NX, HALVES, CAP * SPLIT, piece), BF16),
            pltpu.VMEM((2, NX, NZ, CAP * SPLIT, piece), BF16),
            pltpu.VMEM((NX, 2 * NY, rows, feature), BF16),
            pltpu.VMEM((feature, width), BF16),
            pltpu.VMEM((feature, width), BF16),
            pltpu.VMEM((width, feature), BF16),
            pltpu.VMEM((2 * NY * rows, width), BF16),
            pltpu.VMEM((NX, 2 * NY, rows, feature), BF16),
            pltpu.VMEM((NX, NY, rows, feature), BF16),
            pltpu.VMEM((2, NX, rows, feature // 4), BF16),
            pltpu.VMEM((2, NX, rows, feature // 4), BF16),
            pltpu.VMEM((NX, rows, feature), BF16),
            pltpu.VMEM((NX, rows, feature), BF16),
            pltpu.VMEM((2, NX, NZ, CAP * SPLIT, piece), BF16),
            pltpu.VMEM((2, NX, NZ, CAP * SPLIT, piece), BF16),
            pltpu.VMEM((2, rows * SPLIT, rows * SPLIT), BF16),
            pltpu.VMEM((SPLIT * tok_rows, EXPERTS * CAP * SPLIT), F32),
            dma((6,)),
            dma((2, NX, NZ)),
            dma((2, NX, NZ)),
            dma((2, NX, 8)),
            dma((2, NX, 8)),
            dma((2, NX, 10)),
            dma((2, NX, 10)),
            dma((2, NX, NZ)),
            dma((2, NX, NZ)),
        ],
        compiler_params=pltpu.CompilerParams(
            collective_id=0, has_side_effects=True, vmem_limit_bytes=64 * 1024 * 1024 - 65536
        ),
        name="moe",
    )(tokens, expert_ids.T, gate_quota.T, w_gate, w_up, w_down)


def solution(mesh):
    return jax.shard_map(
        on_device,
        mesh=mesh,
        in_specs=(
            P(("dp", "expert"), None),
            P(("dp", "expert"), None),
            P(("dp", "expert"), None),
            P("expert", None, "dp"),
            P("expert", None, "dp"),
            P("expert", "dp", None),
        ),
        out_specs=P(("dp", "expert"), None),
        check_vma=False,
    )
```

```python
import jax
import jax.numpy as jnp
from jax import lax
from jax.experimental import pallas as pl
from jax.experimental.pallas import tpu as pltpu
from jax.sharding import PartitionSpec as P

MESH = pl.DeviceIdType.MESH
EXPERTS = 8
TOP = 2
CAP = 6
NX = 4
NZ = 8
NY = 4
HALVES = EXPERTS // NX
GROUP = NZ // HALVES
SPLIT = 8
NCHUNK = NX
WIDE_IN = 2
WIDE_OUT = 1
F32 = jnp.float32
BF16 = jnp.bfloat16

STEPS = 17
STAGES = (
    ("rows_wide", (2,), (9,)),
    ("back_1", (0, 2, 3), (10, 15, 16)),
    ("rows_0", (0, 1, 2, 3), (0, 1, 2, 3)),
    ("rows_1", (0, 1, 3), (0, 1, 7)),
    ("ring_1", (0, 2, 3), (6, 11, 13)),
    ("last_1", (0, 2, 3), (7, 13, 14)),
    ("ring_0", (0, 1, 2, 3), (6, 8, 10, 14)),
    ("forward_1", (0, 1, 3), (1, 4, 9)),
    ("back_0", (0, 1, 2, 3), (10, 13, 14, 16)),
    ("far_1", (0, 1, 3), (4, 6, 10)),
    ("compute", (0, 1, 2, 3), (5, 7, 9, 12)),
    ("forward_0", (0, 1, 2, 3), (0, 3, 4, 7)),
    ("back_wide", (1,), (14,)),
    ("last_0", (0, 1, 2, 3), (8, 11, 12, 15)),
    ("ring_wide", (1,), (7,)),
    ("far_0", (0, 1, 2, 3), (3, 6, 8, 9)),
)


def moe_kernel(
    tok_hbm, ids_hbm, quota_hbm, wg_hbm, wu_hbm, wd_hbm, out_ref,
    tok_ref, ids_ref, quota_ref, packed, arr, xall, wg, wu, wd, hid, part, fromcore, ringa, ringb, lasta, lastb, outgo, ret,
    spread, arr_wide, out_wide, ret_wide, fin, fin_in, perm, mix, w_sem, dsend, drecv, gsend, grecv, rsend, rrecv, bsend, brecv, ysend, yrecv,
):
    tok, feature = tok_ref.shape
    half = feature // 2
    quarter = feature // 4
    piece = half // SPLIT
    rows = NZ * CAP
    slots = EXPERTS * CAP
    dp = lax.axis_index("dp")
    ex = lax.axis_index("expert")
    core = lax.rem(dp, 2)
    y = dp // 2
    xx = ex // NZ
    zz = lax.rem(ex, NZ)
    n_ex = NX * NZ
    y_up, y_down, y_far = lax.rem(y + 1, NY), lax.rem(y + NY - 1, NY), lax.rem(y + 2, NY)
    up = y_up * 2 + core
    down = y_down * 2 + core
    far = y_far * 2 + core
    other = y * 2 + (1 - core)

    def both(c):
        return pl.ds(c * half, half)

    def lo(c):
        return pl.ds(c * half, quarter)

    def hi(c):
        return pl.ds(c * half + quarter, quarter)

    barrier = pltpu.get_barrier_semaphore()

    def greet(i, carry):
        pl.semaphore_signal(
            barrier, inc=1, device_id={"expert": lax.rem(ex + i, n_ex)}, device_id_type=MESH
        )
        return carry

    lax.fori_loop(1, n_ex, greet, 0)
    for peer in (up, down, far, other):
        pl.semaphore_signal(barrier, inc=1, device_id={"dp": peer}, device_id_type=MESH)

    first_loads = [
        pltpu.make_async_copy(ids_hbm, ids_ref, w_sem.at[3]),
        pltpu.make_async_copy(quota_hbm, quota_ref, w_sem.at[4]),
        pltpu.make_async_copy(tok_hbm, tok_ref, w_sem.at[5]),
    ]
    for load in first_loads:
        load.start()
    loads = [
        pltpu.make_async_copy(wg_hbm.at[0], wg, w_sem.at[0]),
        pltpu.make_async_copy(wu_hbm.at[0], wu, w_sem.at[1]),
        pltpu.make_async_copy(wd_hbm.at[0], wd, w_sem.at[2]),
    ]
    for load in loads:
        load.start()

    p_row = lax.broadcasted_iota(jnp.int32, (rows * SPLIT, rows * SPLIT), 0)
    p_col = lax.broadcasted_iota(jnp.int32, (rows * SPLIT, rows * SPLIT), 1)
    perm[0] = jnp.where(p_row == (p_col & (SPLIT - 1)) * rows + (p_col >> 3), 1.0, 0.0).astype(BF16)

    for load in first_loads:
        load.wait()

    lanes = SPLIT * tok
    t_row = lax.broadcasted_iota(jnp.int32, (tok, lanes), 0)
    t_col = lax.broadcasted_iota(jnp.int32, (tok, lanes), 1) & (tok - 1)
    eye = lax.broadcasted_iota(jnp.int32, (tok, tok), 0) == lax.broadcasted_iota(
        jnp.int32, (tok, tok), 1
    )

    def as_column(values):
        grid = jnp.where(eye, jnp.broadcast_to(values, (tok, tok)), 0)
        return jnp.broadcast_to(jnp.sum(grid, axis=1, keepdims=True), (tok, lanes))

    ids = [as_column(ids_ref[k : k + 1, :]) for k in range(TOP)]
    quota = [as_column(quota_ref[k : k + 1, :].astype(F32)) for k in range(TOP)]
    place_of, share_of = [], []
    lane_quota = [
        jnp.sum(jnp.where(t_row == t_col, q, 0.0), axis=0, keepdims=True) for q in quota
    ]
    whole_quota = lane_quota[0] + lane_quota[1]
    for k in range(TOP):
        mine = jnp.sum(jnp.where(t_row == t_col, ids[k], 0), axis=0, keepdims=True)
        before = jnp.zeros((tok, lanes), jnp.int32)
        for other_k in range(TOP):
            before = before + jnp.where((ids[other_k] == mine) & (t_row < t_col), 1, 0)
        position = jnp.sum(before, axis=0, keepdims=True)
        ahead = ((mine // HALVES) + NX - xx) & (NX - 1)
        place_of.append((ahead * HALVES + (mine & (HALVES - 1))) * CAP + position)
        share_of.append(lane_quota[k] / whole_quota)
    s_row = lax.broadcasted_iota(jnp.int32, (slots * SPLIT, lanes), 0)
    s_col = lax.broadcasted_iota(jnp.int32, (slots * SPLIT, lanes), 1)
    same_piece = (s_row & (SPLIT - 1)) == (s_col >> (tok.bit_length() - 1))
    hits = [same_piece & ((s_row >> 3) == place_of[k]) for k in range(TOP)]
    pick = (jnp.where(hits[0], 1.0, 0.0) + jnp.where(hits[1], 1.0, 0.0)).astype(BF16)

    for c in range(2):
        stacked = jnp.concatenate(
            [
                tok_ref[:, c * half + o * piece : c * half + (o + 1) * piece]
                for o in range(SPLIT)
            ],
            axis=0,
        )
        chosen = jnp.dot(pick, stacked, preferred_element_type=F32).astype(BF16)
        packed[c] = chosen.reshape(NX, HALVES, CAP * SPLIT, piece)
        arr[c, 0, pl.ds(zz, 1)] = packed[c, 0, pl.ds(zz // GROUP, 1)]

    spread[:, pl.ds(y, 1)] = packed[1, WIDE_IN][:, None]

    pl.semaphore_wait(barrier, n_ex - 1 + 4)

    def to_expert(k, c, dz):
        z_to = lax.rem(zz + dz, NZ)
        x_to = lax.rem(xx + k, NX)
        return pltpu.make_async_remote_copy(
            packed.at[c, k, z_to // GROUP], arr.at[c, k, zz],
            dsend.at[c, k, dz], drecv.at[c, k, zz],
            device_id={"expert": x_to * NZ + z_to}, device_id_type=MESH,
        )

    def to_expert_wide(dz):
        z_to = lax.rem(zz + dz, NZ)
        x_to = lax.rem(xx + WIDE_IN, NX)
        return pltpu.make_async_remote_copy(
            spread.at[z_to // GROUP], arr_wide.at[zz],
            dsend.at[1, WIDE_IN, dz], drecv.at[1, WIDE_IN, zz],
            device_id={"expert": x_to * NZ + z_to}, device_id_type=MESH,
        )

    def expert_arrival_wide(z_from):
        return pltpu.make_async_remote_copy(
            spread.at[0], arr_wide.at[z_from],
            dsend.at[1, WIDE_IN, 0], drecv.at[1, WIDE_IN, z_from],
            device_id={"expert": ex}, device_id_type=MESH,
        )

    def along_y(d):
        peer = lax.rem(y + d, NY) * 2 + core
        return to_dp(
            packed.at[1, WIDE_IN], spread.at[:, y], ysend.at[0, d - 1], yrecv.at[0, d - 1], peer
        )

    def to_owner_wide(dz):
        z_to = lax.rem(zz + dz, NZ)
        x_to = lax.rem(xx + NX - WIDE_OUT, NX)
        return pltpu.make_async_remote_copy(
            out_wide.at[z_to], ret_wide.at[zz],
            bsend.at[1, WIDE_OUT, dz], brecv.at[1, WIDE_OUT, zz],
            device_id={"expert": x_to * NZ + z_to}, device_id_type=MESH,
        )

    def owner_arrival_wide(z_from):
        return pltpu.make_async_remote_copy(
            out_wide.at[0], ret_wide.at[z_from],
            bsend.at[1, WIDE_OUT, 0], brecv.at[1, WIDE_OUT, z_from],
            device_id={"expert": ex}, device_id_type=MESH,
        )

    def home_y(d):
        y_to = lax.rem(y + d, NY)
        return to_dp(
            fin.at[y_to], fin_in.at[d - 1], ysend.at[1, d - 1], yrecv.at[1, d - 1],
            y_to * 2 + core,
        )

    def expert_arrival(k, c, z_from):
        return pltpu.make_async_remote_copy(
            packed.at[c, k, 0], arr.at[c, k, z_from], dsend.at[c, k, 0], drecv.at[c, k, z_from],
            device_id={"expert": ex}, device_id_type=MESH,
        )

    def to_dp(src, dst, send, recv, peer):
        return pltpu.make_async_remote_copy(
            src, dst, send, recv, device_id={"dp": peer}, device_id_type=MESH
        )

    def g_copy(k, c, n):
        block, cols, peer = [
            (dp, both(c), up), (dp, both(c), down), (dp, both(c), other),
            (down, lo(c), up), (up, hi(c), down),
            (down, both(c), other), (up, both(c), other), (far, both(c), other),
        ][n]
        view = xall.at[k, block, :, cols]
        return to_dp(view, view, gsend.at[c, k, n], grecv.at[c, k, n], peer)

    def r_copy(k, c, n):
        send, recv = rsend.at[c, k, n], rrecv.at[c, k, n]
        if n < 4:
            place = [y_far, y_up, y_down, y][n]
            return to_dp(
                part.at[k, place * 2 + (1 - core), :, both(c)],
                fromcore.at[k, place, :, both(c)], send, recv, other,
            )
        src, cols, dst, peer = [
            (far, lo(c), ringa.at[c, k], up),
            (far, hi(c), ringb.at[c, k], down),
            (up, hi(c), lasta.at[k, :, hi(c)], up),
            (down, lo(c), lastb.at[k, :, lo(c)], down),
            (up, lo(c), lasta.at[k, :, lo(c)], up),
            (down, hi(c), lastb.at[k, :, hi(c)], down),
        ][n - 4]
        return to_dp(part.at[k, src, :, cols], dst, send, recv, peer)

    def to_owner(k, c, dz):
        z_to = lax.rem(zz + dz, NZ)
        x_to = lax.rem(xx + NX - k, NX)
        return pltpu.make_async_remote_copy(
            outgo.at[c, k, z_to], ret.at[c, k, zz], bsend.at[c, k, dz], brecv.at[c, k, zz],
            device_id={"expert": x_to * NZ + z_to}, device_id_type=MESH,
        )

    def owner_arrival(k, c, z_from):
        return pltpu.make_async_remote_copy(
            outgo.at[c, k, 0], ret.at[c, k, z_from], bsend.at[c, k, 0], brecv.at[c, k, z_from],
            device_id={"expert": ex}, device_id_type=MESH,
        )

    def each_z(k, action):
        def one(z, inner):
            action(z)
            return inner

        lax.fori_loop(0, NZ, one, 0)

    for d in range(1, NY):
        along_y(d).start()

    def send_all(k, carry):
        for c in range(2):
            def one(dz):
                @pl.when((k != 0) | (dz != 0))
                def _():
                    to_expert(k, c, dz).start()

            if c == 0:
                each_z(k, one)
            else:
                pl.when(k != WIDE_IN)(lambda: each_z(k, one))
        return carry

    lax.fori_loop(0, NCHUNK, send_all, 0)

    perm[1] = jnp.where(p_col == (p_row & (SPLIT - 1)) * rows + (p_row >> 3), 1.0, 0.0).astype(BF16)
    mix_t = jnp.where(hits[0], share_of[0], 0.0) + jnp.where(hits[1], share_of[1], 0.0)
    mix[...] = mix_t.T

    for d in range(1, NY):
        along_y(d).wait_recv()
    each_z(0, lambda dz: to_expert_wide(dz).start())

    def stage_rows(k, c):
        def one(z_from):
            @pl.when((k != 0) | (z_from != zz))
            def _():
                expert_arrival(k, c, z_from).wait_recv()

        each_z(k, one)
        flat = arr[c, k].reshape(NZ * CAP * SPLIT, piece)
        sorted_rows = jnp.dot(perm[0], flat, preferred_element_type=F32).astype(BF16)
        for o in range(SPLIT):
            xall[k, dp, :, c * half + o * piece : c * half + (o + 1) * piece] = sorted_rows[
                o * rows : (o + 1) * rows
            ]
        for n in range(3):
            g_copy(k, c, n).start()

    def stage_rows_wide():
        each_z(0, lambda z_from: expert_arrival_wide(z_from).wait_recv())
        for n, place in ((2, y), (5, y_down), (6, y_up), (7, y_far)):
            flat = arr_wide[:, pl.ds(place, 1)].reshape(NZ * CAP * SPLIT, piece)
            sorted_rows = jnp.dot(perm[0], flat, preferred_element_type=F32).astype(BF16)
            for o in range(SPLIT):
                xall[WIDE_IN, place * 2 + core, :, half + o * piece : half + (o + 1) * piece] = (
                    sorted_rows[o * rows : (o + 1) * rows]
                )
            g_copy(WIDE_IN, 1, n).start()

    def stage_forward(k, c):
        g_copy(k, c, 0).wait_recv()
        g_copy(k, c, 3).start()
        g_copy(k, c, 5).start()
        g_copy(k, c, 1).wait_recv()
        g_copy(k, c, 4).start()
        g_copy(k, c, 6).start()

    def stage_far(k, c):
        g_copy(k, c, 3).wait_recv()
        g_copy(k, c, 4).wait_recv()
        g_copy(k, c, 7).start()

    def stage_compute(k):
        for c in range(2):
            for n in (2, 5, 6, 7):
                g_copy(k, c, n).wait_recv()

        @pl.when(k == 0)
        def _():
            for load in loads:
                load.wait()

        for m in range(2):
            x_in = xall[k, m * NY : (m + 1) * NY].reshape(NY * rows, feature)
            gate = jnp.dot(x_in, wg[...], preferred_element_type=F32)
            up_act = jnp.dot(x_in, wu[...], preferred_element_type=F32)
            hid[m * NY * rows : (m + 1) * NY * rows] = (
                gate * (1.0 / (1.0 + jnp.exp(-gate))) * up_act
            ).astype(BF16)

        wide = half // 4
        for c in range(2):
            def down_block(n, carry):
                cols = pl.ds(pl.multiple_of(c * half + n * wide, wide), wide)
                got = jnp.dot(hid[...], wd[:, cols], preferred_element_type=F32).astype(BF16)
                part[k, :, :, cols] = got.reshape(2 * NY, rows, wide)
                return carry

            lax.fori_loop(0, 4, down_block, 0)
            for n in range(4):
                r_copy(k, c, n).start()

    def join(k, c, place):
        mine = place * 2 + core
        cols = both(c)
        total = part[k, mine, :, cols].astype(F32) + fromcore[k, place, :, cols].astype(F32)
        part[k, mine, :, cols] = total.astype(BF16)

    def stage_ring(k, c):
        r_copy(k, c, 0).wait_recv()
        join(k, c, y_far)
        r_copy(k, c, 4).start()
        r_copy(k, c, 5).start()
        r_copy(k, c, 1).wait_recv()
        join(k, c, y_up)
        r_copy(k, c, 6).start()
        r_copy(k, c, 2).wait_recv()
        join(k, c, y_down)
        r_copy(k, c, 7).start()

    def to_pieces(k, c, place, extra):
        pieces = []
        for o in range(SPLIT):
            cols = slice(c * half + o * piece, c * half + (o + 1) * piece)
            total = part[k, place * 2 + core, :, cols].astype(F32)
            for more in [fromcore.at[k, place]] + extra:
                total = total + more[:, cols].astype(F32)
            pieces.append(total.astype(BF16))
        block = jnp.concatenate(pieces, axis=0)
        return jnp.dot(perm[1], block, preferred_element_type=F32).astype(BF16)

    def stage_ring_wide():
        for n, place in ((0, y_far), (1, y_up), (2, y_down), (3, y)):
            r_copy(WIDE_OUT, 1, n).wait_recv()
            sorted_rows = to_pieces(WIDE_OUT, 1, place, [])
            out_wide[:, pl.ds(place, 1)] = sorted_rows.reshape(NZ, 1, CAP * SPLIT, piece)
        each_z(0, lambda dz: to_owner_wide(dz).start())

    def stage_back_wide():
        each_z(0, lambda z_from: owner_arrival_wide(z_from).wait_recv())
        for place in range(NY):
            for h in range(HALVES):
                total = ret_wide[h * GROUP, place].astype(F32)
                for g in range(1, GROUP):
                    total = total + ret_wide[h * GROUP + g, place].astype(F32)
                fin[place, h] = total.astype(BF16)
        for d in range(1, NY):
            home_y(d).start()

    def stage_last(k, c):
        r_copy(k, c, 4).wait_recv()
        part[k, up, :, lo(c)] = (
            part[k, up, :, lo(c)].astype(F32) + ringa[c, k].astype(F32)
        ).astype(BF16)
        r_copy(k, c, 8).start()
        r_copy(k, c, 5).wait_recv()
        part[k, down, :, hi(c)] = (
            part[k, down, :, hi(c)].astype(F32) + ringb[c, k].astype(F32)
        ).astype(BF16)
        r_copy(k, c, 9).start()

    def stage_back(k, c):
        r_copy(k, c, 3).wait_recv()
        for n in (6, 7, 8, 9):
            r_copy(k, c, n).wait_recv()
        sorted_rows = to_pieces(k, c, y, [lasta.at[k], lastb.at[k]])
        outgo[c, k] = sorted_rows.reshape(NZ, CAP * SPLIT, piece)

        def one(dz):
            @pl.when((k != 0) | (dz != 0))
            def _():
                to_owner(k, c, dz).start()

        each_z(k, one)

        @pl.when(k == 0)
        def _():
            ret[c, 0, pl.ds(zz, 1)] = outgo[c, 0, pl.ds(zz, 1)]

    todo = {
        "rows": stage_rows, "forward": stage_forward, "far": stage_far,
        "ring": stage_ring, "last": stage_last, "back": stage_back,
    }

    def run(stage, k):
        name, _, c = stage.partition("_")
        if stage == "compute":
            stage_compute(k)
        elif stage == "rows_wide":
            stage_rows_wide()
        elif stage == "ring_wide":
            stage_ring_wide()
        elif stage == "back_wide":
            stage_back_wide()
        else:
            todo[name](k, int(c))

    def step(i, carry):
        for stage, chunks, due in STAGES:
            k = chunks[0]
            for n in range(1, len(due)):
                k = k + jnp.where(i >= due[n], chunks[n] - chunks[n - 1], 0)
            now = i == due[0]
            for at in due[1:]:
                now = now | (i == at)

            @pl.when(now)
            def _(stage=stage, k=k):
                run(stage, k)

        return carry

    lax.fori_loop(0, STEPS, step, 0)

    sums = []
    for c in range(2):
        def arrived(k, carry):
            def one(z):
                @pl.when((k != 0) | (z != zz))
                def _():
                    owner_arrival(k, c, z).wait_recv()

            if c == 0:
                each_z(k, one)
            else:
                pl.when(k != WIDE_OUT)(lambda: each_z(k, one))
            return carry

        lax.fori_loop(0, NCHUNK, arrived, 0)
        if c == 1:
            for d in range(1, NY):
                home_y(d).wait_recv()
        sums = []
        for k in range(NX):
            for h in range(HALVES):
                if (c, k) == (1, WIDE_OUT):
                    total = fin[pl.ds(y, 1), h].astype(F32).reshape(CAP * SPLIT, piece)
                    for d in range(NY - 1):
                        total = total + fin_in[d, h].astype(F32)
                else:
                    total = ret[c, k, h * GROUP].astype(F32)
                    for g in range(1, GROUP):
                        total = total + ret[c, k, h * GROUP + g].astype(F32)
                sums.append(total)
        mixed = jnp.dot(
            mix[...], jnp.concatenate(sums, axis=0),
            preferred_element_type=F32, precision=lax.Precision.HIGHEST,
        ).astype(BF16)
        for o in range(SPLIT):
            out_ref[:, c * half + o * piece : c * half + (o + 1) * piece] = mixed[
                o * tok : (o + 1) * tok
            ]

    def drain(k, carry):
        for c in range(2):
            def one_in(z):
                @pl.when((k != 0) | (z != 0))
                def _():
                    to_expert(k, c, z).wait_send()

            def one_out(z):
                @pl.when((k != 0) | (z != 0))
                def _():
                    to_owner(k, c, z).wait_send()

            def narrow_in():
                each_z(k, one_in)
                for n in (0, 1, 3, 4):
                    g_copy(k, c, n).wait_send()

            def narrow_out():
                each_z(k, one_out)
                for n in range(4, 10):
                    r_copy(k, c, n).wait_send()

            if c == 0:
                narrow_in()
                narrow_out()
            else:
                pl.when(k != WIDE_IN)(narrow_in)
                pl.when(k != WIDE_OUT)(narrow_out)
            for n in (2, 5, 6, 7):
                g_copy(k, c, n).wait_send()
            for n in range(4):
                r_copy(k, c, n).wait_send()
        return carry

    lax.fori_loop(0, NCHUNK, drain, 0)

    def drain_wide(dz):
        to_expert_wide(dz).wait_send()
        to_owner_wide(dz).wait_send()

    each_z(0, drain_wide)
    for d in range(1, NY):
        along_y(d).wait_send()
        home_y(d).wait_send()


def on_device(tokens, expert_ids, gate_quota, w_gate, w_up, w_down):
    tok_rows, feature = tokens.shape
    width = w_gate.shape[2]
    half = feature // 2
    piece = half // SPLIT
    rows = NZ * CAP
    whole = pl.BlockSpec(memory_space=pltpu.VMEM)
    anywhere = pl.BlockSpec(memory_space=pl.ANY)
    dma = pltpu.SemaphoreType.DMA
    return pl.pallas_call(
        moe_kernel,
        out_shape=jax.ShapeDtypeStruct((tok_rows, feature), BF16),
        in_specs=[anywhere] * 6,
        out_specs=whole,
        scratch_shapes=[
            pltpu.VMEM((tok_rows, feature), BF16),
            pltpu.VMEM((TOP, tok_rows), jnp.int32),
            pltpu.VMEM((TOP, tok_rows), jnp.int32),
            pltpu.VMEM((2, NX, HALVES, CAP * SPLIT, piece), BF16),
            pltpu.VMEM((2, NX, NZ, CAP * SPLIT, piece), BF16),
            pltpu.VMEM((NX, 2 * NY, rows, feature), BF16),
            pltpu.VMEM((feature, width), BF16),
            pltpu.VMEM((feature, width), BF16),
            pltpu.VMEM((width, feature), BF16),
            pltpu.VMEM((2 * NY * rows, width), BF16),
            pltpu.VMEM((NX, 2 * NY, rows, feature), BF16),
            pltpu.VMEM((NX, NY, rows, feature), BF16),
            pltpu.VMEM((2, NX, rows, feature // 4), BF16),
            pltpu.VMEM((2, NX, rows, feature // 4), BF16),
            pltpu.VMEM((NX, rows, feature), BF16),
            pltpu.VMEM((NX, rows, feature), BF16),
            pltpu.VMEM((2, NX, NZ, CAP * SPLIT, piece), BF16),
            pltpu.VMEM((2, NX, NZ, CAP * SPLIT, piece), BF16),
            pltpu.VMEM((HALVES, NY, CAP * SPLIT, piece), BF16),
            pltpu.VMEM((NZ, NY, CAP * SPLIT, piece), BF16),
            pltpu.VMEM((NZ, NY, CAP * SPLIT, piece), BF16),
            pltpu.VMEM((NZ, NY, CAP * SPLIT, piece), BF16),
            pltpu.VMEM((NY, HALVES, CAP * SPLIT, piece), BF16),
            pltpu.VMEM((NY - 1, HALVES, CAP * SPLIT, piece), BF16),
            pltpu.VMEM((2, rows * SPLIT, rows * SPLIT), BF16),
            pltpu.VMEM((SPLIT * tok_rows, EXPERTS * CAP * SPLIT), F32),
            dma((6,)),
            dma((2, NX, NZ)),
            dma((2, NX, NZ)),
            dma((2, NX, 8)),
            dma((2, NX, 8)),
            dma((2, NX, 10)),
            dma((2, NX, 10)),
            dma((2, NX, NZ)),
            dma((2, NX, NZ)),
            dma((2, NY - 1)),
            dma((2, NY - 1)),
        ],
        compiler_params=pltpu.CompilerParams(
            collective_id=0, has_side_effects=True, vmem_limit_bytes=64 * 1024 * 1024 - 65536
        ),
        name="moe",
    )(tokens, expert_ids.T, gate_quota.T, w_gate, w_up, w_down)


def solution(mesh):
    return jax.shard_map(
        on_device,
        mesh=mesh,
        in_specs=(
            P(("dp", "expert"), None),
            P(("dp", "expert"), None),
            P(("dp", "expert"), None),
            P("expert", None, "dp"),
            P("expert", None, "dp"),
            P("expert", "dp", None),
        ),
        out_specs=P(("dp", "expert"), None),
        check_vma=False,
    )
```

```python
import jax
import jax.numpy as jnp
from jax import lax
from jax.experimental import pallas as pl
from jax.experimental.pallas import tpu as pltpu
from jax.sharding import PartitionSpec as P

MESH = pl.DeviceIdType.MESH
EXPERTS = 8
TOP = 2
CAP = 6
NX = 4
NZ = 8
NY = 4
HALVES = EXPERTS // NX
GROUP = NZ // HALVES
SPLIT = 8
UNITS = (1, 1)
NC = len(UNITS)
WIDE = NC - 1
NCHUNK = NX
WIDE_IN = 1
WIDE_OUT = 1
F32 = jnp.float32
BF16 = jnp.bfloat16
FINAL = (
    (0, 0),
    (0, 1),
    (1, 0),
    (2, 0),
    (3, 0),
    (1, 1),
    (2, 1),
    (3, 1),
)

SEGMENTS = (
    (
        ("rows_0", 0),
        ("rows_1", 0),
        ("rows_0", 1),
        ("forward_0", 0),
        ("rows_0", 2),
        ("far_0", 0),
        ("forward_1", 0),
        ("forward_0", 1),
        ("rows_1", 2),
        ("far_1", 0),
        ("forward_0", 2),
        ("rows_0", 3),
    ),
    (
        ("far_0", 1),
        ("ring_0", 0),
        ("rows_1", 3),
        ("last_0", 0),
        ("rows_wide", 1),
        ("forward_1", 2),
        ("far_0", 2),
        ("ring_1", 0),
    ),
    (
        ("forward_0", 3),
        ("back_0", 0),
        ("last_1", 0),
        ("forward_1", 3),
        ("ring_wide", 1),
        ("far_1", 2),
        ("ring_0", 1),
    ),
    (
        ("back_1", 0),
        ("far_0", 3),
        ("ring_0", 2),
        ("far_1", 3),
        ("last_0", 1),
    ),
    (
        ("last_0", 2),
        ("ring_0", 3),
        ("ring_1", 2),
        ("back_0", 1),
        ("last_0", 3),
        ("last_1", 2),
        ("back_0", 2),
        ("ring_1", 3),
        ("back_0", 3),
        ("back_wide", 1),
        ("back_1", 2),
        ("last_1", 3),
        ("back_1", 3),
    ),
)


def unit_columns(feature):
    wid = [feature * u // sum(UNITS) for u in UNITS]
    return wid, [sum(wid[:c]) for c in range(NC)]


def moe_kernel(
    tok_hbm, ids_hbm, quota_hbm, wg_hbm, wu_hbm, wd_hbm, out_ref,
    tok_ref, ids_ref, quota_ref, packed, arr, xall, wg, wu, wd, hid, part, fromcore, ringa, ringb, lasta, lastb, outgo, ret,
    spread, arr_wide, out_wide, ret_wide, fin, fin_in, perm, mix, acc, w_sem, dsend, drecv, gsend, grecv, rsend, rrecv, bsend, brecv, ysend, yrecv,
):
    tok, feature = tok_ref.shape
    wid, off = unit_columns(feature)
    rows = NZ * CAP
    slots = EXPERTS * CAP
    dp = lax.axis_index("dp")
    ex = lax.axis_index("expert")
    core = lax.rem(dp, 2)
    y = dp // 2
    xx = ex // NZ
    zz = lax.rem(ex, NZ)
    n_ex = NX * NZ
    y_up, y_down, y_far = lax.rem(y + 1, NY), lax.rem(y + NY - 1, NY), lax.rem(y + 2, NY)
    up = y_up * 2 + core
    down = y_down * 2 + core
    far = y_far * 2 + core
    other = y * 2 + (1 - core)

    def both(c):
        return pl.ds(off[c], wid[c])

    def lo(c):
        return pl.ds(off[c], wid[c] // 2)

    def hi(c):
        return pl.ds(off[c] + wid[c] // 2, wid[c] // 2)

    def piece_cols(c, o):
        piece = wid[c] // SPLIT
        return slice(off[c] + o * piece, off[c] + (o + 1) * piece)

    barrier = pltpu.get_barrier_semaphore()

    def greet(i, carry):
        pl.semaphore_signal(
            barrier, inc=1, device_id={"expert": lax.rem(ex + i, n_ex)}, device_id_type=MESH
        )
        return carry

    lax.fori_loop(1, n_ex, greet, 0)
    for peer in (up, down, far, other):
        pl.semaphore_signal(barrier, inc=1, device_id={"dp": peer}, device_id_type=MESH)

    first_loads = [
        pltpu.make_async_copy(ids_hbm, ids_ref, w_sem.at[3]),
        pltpu.make_async_copy(quota_hbm, quota_ref, w_sem.at[4]),
        pltpu.make_async_copy(tok_hbm, tok_ref, w_sem.at[5]),
    ]
    for load in first_loads:
        load.start()
    loads = [
        pltpu.make_async_copy(wg_hbm.at[0], wg, w_sem.at[0]),
        pltpu.make_async_copy(wu_hbm.at[0], wu, w_sem.at[1]),
        pltpu.make_async_copy(wd_hbm.at[0], wd, w_sem.at[2]),
    ]
    for load in loads:
        load.start()

    p_row = lax.broadcasted_iota(jnp.int32, (rows * SPLIT, rows * SPLIT), 0)
    p_col = lax.broadcasted_iota(jnp.int32, (rows * SPLIT, rows * SPLIT), 1)
    perm[0] = jnp.where(p_row == (p_col & (SPLIT - 1)) * rows + (p_col >> 3), 1.0, 0.0).astype(BF16)

    for load in first_loads:
        load.wait()

    lanes = SPLIT * tok
    t_row = lax.broadcasted_iota(jnp.int32, (tok, lanes), 0)
    t_col = lax.broadcasted_iota(jnp.int32, (tok, lanes), 1) & (tok - 1)
    eye = lax.broadcasted_iota(jnp.int32, (tok, tok), 0) == lax.broadcasted_iota(
        jnp.int32, (tok, tok), 1
    )

    def as_column(values):
        grid = jnp.where(eye, jnp.broadcast_to(values, (tok, tok)), 0)
        return jnp.broadcast_to(jnp.sum(grid, axis=1, keepdims=True), (tok, lanes))

    ids = [as_column(ids_ref[k : k + 1, :]) for k in range(TOP)]
    quota = [as_column(quota_ref[k : k + 1, :].astype(F32)) for k in range(TOP)]
    place_of, share_of = [], []
    lane_quota = [
        jnp.sum(jnp.where(t_row == t_col, q, 0.0), axis=0, keepdims=True) for q in quota
    ]
    whole_quota = lane_quota[0] + lane_quota[1]
    for k in range(TOP):
        mine = jnp.sum(jnp.where(t_row == t_col, ids[k], 0), axis=0, keepdims=True)
        before = jnp.zeros((tok, lanes), jnp.int32)
        for other_k in range(TOP):
            before = before + jnp.where((ids[other_k] == mine) & (t_row < t_col), 1, 0)
        position = jnp.sum(before, axis=0, keepdims=True)
        ahead = ((mine // HALVES) + NX - xx) & (NX - 1)
        place_of.append((ahead * HALVES + (mine & (HALVES - 1))) * CAP + position)
        share_of.append(lane_quota[k] / whole_quota)
    s_row = lax.broadcasted_iota(jnp.int32, (slots * SPLIT, lanes), 0)
    s_col = lax.broadcasted_iota(jnp.int32, (slots * SPLIT, lanes), 1)
    same_piece = (s_row & (SPLIT - 1)) == (s_col >> (tok.bit_length() - 1))
    hits = [same_piece & ((s_row >> 3) == place_of[k]) for k in range(TOP)]
    pick = (jnp.where(hits[0], 1.0, 0.0) + jnp.where(hits[1], 1.0, 0.0)).astype(BF16)

    for c in range(NC):
        stacked = jnp.concatenate([tok_ref[:, piece_cols(c, o)] for o in range(SPLIT)], axis=0)
        chosen = jnp.dot(pick, stacked, preferred_element_type=F32).astype(BF16)
        packed[c][...] = chosen.reshape(packed[c].shape)
        arr[c][0, pl.ds(zz, 1)] = packed[c][0, pl.ds(zz // GROUP, 1)]

    spread[:, pl.ds(y, 1)] = packed[WIDE][WIDE_IN][:, None]

    pl.semaphore_wait(barrier, n_ex - 1 + 4)

    def to_expert(k, c, dz):
        z_to = lax.rem(zz + dz, NZ)
        x_to = lax.rem(xx + k, NX)
        return pltpu.make_async_remote_copy(
            packed[c].at[k, z_to // GROUP], arr[c].at[k, zz],
            dsend.at[c, k, dz], drecv.at[c, k, zz],
            device_id={"expert": x_to * NZ + z_to}, device_id_type=MESH,
        )

    def to_expert_wide(dz):
        z_to = lax.rem(zz + dz, NZ)
        x_to = lax.rem(xx + WIDE_IN, NX)
        return pltpu.make_async_remote_copy(
            spread.at[z_to // GROUP], arr_wide.at[zz],
            dsend.at[WIDE, WIDE_IN, dz], drecv.at[WIDE, WIDE_IN, zz],
            device_id={"expert": x_to * NZ + z_to}, device_id_type=MESH,
        )

    def expert_arrival_wide(z_from):
        return pltpu.make_async_remote_copy(
            spread.at[0], arr_wide.at[z_from],
            dsend.at[WIDE, WIDE_IN, 0], drecv.at[WIDE, WIDE_IN, z_from],
            device_id={"expert": ex}, device_id_type=MESH,
        )

    def along_y(d):
        peer = lax.rem(y + d, NY) * 2 + core
        return to_dp(
            packed[WIDE].at[WIDE_IN], spread.at[:, y], ysend.at[0, d - 1], yrecv.at[0, d - 1], peer
        )

    def to_owner_wide(dz):
        z_to = lax.rem(zz + dz, NZ)
        x_to = lax.rem(xx + NX - WIDE_OUT, NX)
        return pltpu.make_async_remote_copy(
            out_wide.at[z_to], ret_wide.at[zz],
            bsend.at[WIDE, WIDE_OUT, dz], brecv.at[WIDE, WIDE_OUT, zz],
            device_id={"expert": x_to * NZ + z_to}, device_id_type=MESH,
        )

    def owner_arrival_wide(z_from):
        return pltpu.make_async_remote_copy(
            out_wide.at[0], ret_wide.at[z_from],
            bsend.at[WIDE, WIDE_OUT, 0], brecv.at[WIDE, WIDE_OUT, z_from],
            device_id={"expert": ex}, device_id_type=MESH,
        )

    def home_y(d):
        y_to = lax.rem(y + d, NY)
        return to_dp(
            fin.at[y_to], fin_in.at[d - 1], ysend.at[1, d - 1], yrecv.at[1, d - 1],
            y_to * 2 + core,
        )

    def expert_arrival(k, c, z_from):
        return pltpu.make_async_remote_copy(
            packed[c].at[k, 0], arr[c].at[k, z_from], dsend.at[c, k, 0], drecv.at[c, k, z_from],
            device_id={"expert": ex}, device_id_type=MESH,
        )

    def to_dp(src, dst, send, recv, peer):
        return pltpu.make_async_remote_copy(
            src, dst, send, recv, device_id={"dp": peer}, device_id_type=MESH
        )

    def g_copy(k, c, n):
        block, cols, peer = [
            (dp, both(c), up), (dp, both(c), down), (dp, both(c), other),
            (down, lo(c), up), (up, hi(c), down),
            (down, both(c), other), (up, both(c), other), (far, both(c), other),
        ][n]
        view = xall.at[k, block, :, cols]
        return to_dp(view, view, gsend.at[c, k, n], grecv.at[c, k, n], peer)

    def r_copy(k, c, n):
        send, recv = rsend.at[c, k, n], rrecv.at[c, k, n]
        if n < 4:
            place = [y_far, y_up, y_down, y][n]
            return to_dp(
                part.at[k, place * 2 + (1 - core), :, both(c)],
                fromcore.at[k, place, :, both(c)], send, recv, other,
            )
        src, cols, dst, peer = [
            (far, lo(c), ringa[c].at[k], up),
            (far, hi(c), ringb[c].at[k], down),
            (up, hi(c), lasta.at[k, :, hi(c)], up),
            (down, lo(c), lastb.at[k, :, lo(c)], down),
            (up, lo(c), lasta.at[k, :, lo(c)], up),
            (down, hi(c), lastb.at[k, :, hi(c)], down),
        ][n - 4]
        return to_dp(part.at[k, src, :, cols], dst, send, recv, peer)

    def to_owner(k, c, dz):
        z_to = lax.rem(zz + dz, NZ)
        x_to = lax.rem(xx + NX - k, NX)
        return pltpu.make_async_remote_copy(
            outgo[c].at[k, z_to], ret[c].at[k, zz], bsend.at[c, k, dz], brecv.at[c, k, zz],
            device_id={"expert": x_to * NZ + z_to}, device_id_type=MESH,
        )

    def owner_arrival(k, c, z_from):
        return pltpu.make_async_remote_copy(
            outgo[c].at[k, 0], ret[c].at[k, z_from], bsend.at[c, k, 0], brecv.at[c, k, z_from],
            device_id={"expert": ex}, device_id_type=MESH,
        )

    def each_z(k, action):
        def one(z, inner):
            action(z)
            return inner

        lax.fori_loop(0, NZ, one, 0)

    for d in range(1, NY):
        along_y(d).start()

    def send_all(k, carry):
        for c in range(NC):
            def one(dz):
                @pl.when((k != 0) | (dz != 0))
                def _():
                    to_expert(k, c, dz).start()

            if c != WIDE:
                each_z(k, one)
            else:
                pl.when(k != WIDE_IN)(lambda: each_z(k, one))
        return carry

    lax.fori_loop(0, NCHUNK, send_all, 0)

    perm[1] = jnp.where(p_col == (p_row & (SPLIT - 1)) * rows + (p_row >> 3), 1.0, 0.0).astype(BF16)
    mix_t = jnp.where(hits[0], share_of[0], 0.0) + jnp.where(hits[1], share_of[1], 0.0)
    share = mix_t.shape[0] // NX
    for k in range(NX):
        mix[k] = mix_t[k * share : (k + 1) * share].T

    for d in range(1, NY):
        along_y(d).wait_recv()
    each_z(0, lambda dz: to_expert_wide(dz).start())

    def stage_rows(k, c):
        def one(z_from):
            @pl.when((k != 0) | (z_from != zz))
            def _():
                expert_arrival(k, c, z_from).wait_recv()

        each_z(k, one)
        flat = arr[c][k].reshape(NZ * CAP * SPLIT, wid[c] // SPLIT)
        sorted_rows = jnp.dot(perm[0], flat, preferred_element_type=F32).astype(BF16)
        for o in range(SPLIT):
            xall[k, dp, :, piece_cols(c, o)] = sorted_rows[o * rows : (o + 1) * rows]
        for n in range(3):
            g_copy(k, c, n).start()

    def stage_rows_wide():
        each_z(0, lambda z_from: expert_arrival_wide(z_from).wait_recv())
        for n, place in ((2, y), (5, y_down), (6, y_up), (7, y_far)):
            flat = arr_wide[:, pl.ds(place, 1)].reshape(NZ * CAP * SPLIT, wid[WIDE] // SPLIT)
            sorted_rows = jnp.dot(perm[0], flat, preferred_element_type=F32).astype(BF16)
            for o in range(SPLIT):
                xall[WIDE_IN, place * 2 + core, :, piece_cols(WIDE, o)] = sorted_rows[
                    o * rows : (o + 1) * rows
                ]
            g_copy(WIDE_IN, WIDE, n).start()

    def stage_forward(k, c):
        g_copy(k, c, 0).wait_recv()
        g_copy(k, c, 3).start()
        g_copy(k, c, 5).start()
        g_copy(k, c, 1).wait_recv()
        g_copy(k, c, 4).start()
        g_copy(k, c, 6).start()

    def stage_far(k, c):
        g_copy(k, c, 3).wait_recv()
        g_copy(k, c, 4).wait_recv()
        g_copy(k, c, 7).start()

    def stage_compute(k):
        for c in range(NC):
            for n in (2, 5, 6, 7):
                g_copy(k, c, n).wait_recv()

        @pl.when(k == 0)
        def _():
            for load in loads:
                load.wait()

        for m in range(2):
            x_in = xall[k, m * NY : (m + 1) * NY].reshape(NY * rows, feature)
            gate = jnp.dot(x_in, wg[...], preferred_element_type=F32)
            up_act = jnp.dot(x_in, wu[...], preferred_element_type=F32)
            hid[m * NY * rows : (m + 1) * NY * rows] = (
                gate * (1.0 / (1.0 + jnp.exp(-gate))) * up_act
            ).astype(BF16)

        wide = min(wid) // 2
        for c in range(NC):
            def down_block(n, carry):
                cols = pl.ds(pl.multiple_of(off[c] + n * wide, wide), wide)
                got = jnp.dot(hid[...], wd[:, cols], preferred_element_type=F32).astype(BF16)
                part[k, :, :, cols] = got.reshape(2 * NY, rows, wide)
                return carry

            lax.fori_loop(0, wid[c] // wide, down_block, 0)
            for n in range(4):
                r_copy(k, c, n).start()

    def join(k, c, place):
        mine = place * 2 + core
        cols = both(c)
        total = part[k, mine, :, cols].astype(F32) + fromcore[k, place, :, cols].astype(F32)
        part[k, mine, :, cols] = total.astype(BF16)

    def stage_ring(k, c):
        r_copy(k, c, 0).wait_recv()
        join(k, c, y_far)
        r_copy(k, c, 4).start()
        r_copy(k, c, 5).start()
        r_copy(k, c, 1).wait_recv()
        join(k, c, y_up)
        r_copy(k, c, 6).start()
        r_copy(k, c, 2).wait_recv()
        join(k, c, y_down)
        r_copy(k, c, 7).start()

    def to_pieces(k, c, place, extra):
        pieces = []
        for o in range(SPLIT):
            cols = piece_cols(c, o)
            total = part[k, place * 2 + core, :, cols].astype(F32)
            for more in [fromcore.at[k, place]] + extra:
                total = total + more[:, cols].astype(F32)
            pieces.append(total.astype(BF16))
        block = jnp.concatenate(pieces, axis=0)
        return jnp.dot(perm[1], block, preferred_element_type=F32).astype(BF16)

    def stage_ring_wide():
        for n, place in ((0, y_far), (1, y_up), (2, y_down), (3, y)):
            r_copy(WIDE_OUT, WIDE, n).wait_recv()
            sorted_rows = to_pieces(WIDE_OUT, WIDE, place, [])
            out_wide[:, pl.ds(place, 1)] = sorted_rows.reshape(
                NZ, 1, CAP * SPLIT, wid[WIDE] // SPLIT
            )
        each_z(0, lambda dz: to_owner_wide(dz).start())

    def stage_back_wide():
        each_z(0, lambda z_from: owner_arrival_wide(z_from).wait_recv())
        for place in range(NY):
            for h in range(HALVES):
                total = ret_wide[h * GROUP, place].astype(F32)
                for g in range(1, GROUP):
                    total = total + ret_wide[h * GROUP + g, place].astype(F32)
                fin[place, h] = total.astype(BF16)
        for d in range(1, NY):
            home_y(d).start()

    def stage_last(k, c):
        r_copy(k, c, 4).wait_recv()
        part[k, up, :, lo(c)] = (
            part[k, up, :, lo(c)].astype(F32) + ringa[c][k].astype(F32)
        ).astype(BF16)
        r_copy(k, c, 8).start()
        r_copy(k, c, 5).wait_recv()
        part[k, down, :, hi(c)] = (
            part[k, down, :, hi(c)].astype(F32) + ringb[c][k].astype(F32)
        ).astype(BF16)
        r_copy(k, c, 9).start()

    def stage_back(k, c):
        r_copy(k, c, 3).wait_recv()
        for n in (6, 7, 8, 9):
            r_copy(k, c, n).wait_recv()
        sorted_rows = to_pieces(k, c, y, [lasta.at[k], lastb.at[k]])
        outgo[c][k] = sorted_rows.reshape(NZ, CAP * SPLIT, wid[c] // SPLIT)

        def one(dz):
            @pl.when((k != 0) | (dz != 0))
            def _():
                to_owner(k, c, dz).start()

        each_z(k, one)

        @pl.when(k == 0)
        def _():
            ret[c][0, pl.ds(zz, 1)] = outgo[c][0, pl.ds(zz, 1)]

    todo = {
        "rows": stage_rows, "forward": stage_forward, "far": stage_far,
        "ring": stage_ring, "last": stage_last, "back": stage_back,
    }

    def run(stage, k):
        name, _, c = stage.partition("_")
        if stage == "rows_wide":
            stage_rows_wide()
        elif stage == "ring_wide":
            stage_ring_wide()
        elif stage == "back_wide":
            stage_back_wide()
        else:
            todo[name](k, int(c))

    def step(i, carry):
        for at, segment in enumerate(SEGMENTS):
            @pl.when(i == at)
            def _(segment=segment):
                for stage, k in segment:
                    run(stage, k)

        @pl.when(i < NCHUNK)
        def _():
            stage_compute(i)

        return carry

    lax.fori_loop(0, NCHUNK + 1, step, 0)

    for at, (k, c) in enumerate(FINAL):
        if (c, k) == (WIDE, WIDE_OUT):
            for d in range(1, NY):
                home_y(d).wait_recv()
        else:
            def one(z):
                if k == 0:
                    pl.when(z != zz)(lambda: owner_arrival(k, c, z).wait_recv())
                else:
                    owner_arrival(k, c, z).wait_recv()

            each_z(k, one)
        sums = []
        for h in range(HALVES):
            if (c, k) == (WIDE, WIDE_OUT):
                total = fin[pl.ds(y, 1), h].astype(F32).reshape(fin.shape[2:])
                for d in range(NY - 1):
                    total = total + fin_in[d, h].astype(F32)
            else:
                total = ret[c][k, h * GROUP].astype(F32)
                for g in range(1, GROUP):
                    total = total + ret[c][k, h * GROUP + g].astype(F32)
            sums.append(total)
        mixed = jnp.dot(
            mix[k], jnp.concatenate(sums, axis=0),
            preferred_element_type=F32, precision=lax.Precision.HIGHEST,
        )
        seen = [kk for kk, cc in FINAL[:at] if cc == c]
        if seen:
            mixed = mixed + acc[c][...]
        if len(seen) < NCHUNK - 1:
            acc[c][...] = mixed
        else:
            mixed = mixed.astype(BF16)
            for o in range(SPLIT):
                out_ref[:, piece_cols(c, o)] = mixed[o * tok : (o + 1) * tok]

    def drain(k, carry):
        for c in range(NC):
            def one_in(z):
                @pl.when((k != 0) | (z != 0))
                def _():
                    to_expert(k, c, z).wait_send()

            def one_out(z):
                @pl.when((k != 0) | (z != 0))
                def _():
                    to_owner(k, c, z).wait_send()

            def narrow_in():
                each_z(k, one_in)
                for n in (0, 1, 3, 4):
                    g_copy(k, c, n).wait_send()

            def narrow_out():
                each_z(k, one_out)
                for n in range(4, 10):
                    r_copy(k, c, n).wait_send()

            if c != WIDE:
                narrow_in()
                narrow_out()
            else:
                pl.when(k != WIDE_IN)(narrow_in)
                pl.when(k != WIDE_OUT)(narrow_out)
            for n in (2, 5, 6, 7):
                g_copy(k, c, n).wait_send()
            for n in range(4):
                r_copy(k, c, n).wait_send()
        return carry

    lax.fori_loop(0, NCHUNK, drain, 0)

    def drain_wide(dz):
        to_expert_wide(dz).wait_send()
        to_owner_wide(dz).wait_send()

    each_z(0, drain_wide)
    for d in range(1, NY):
        along_y(d).wait_send()
        home_y(d).wait_send()


def on_device(tokens, expert_ids, gate_quota, w_gate, w_up, w_down):
    tok_rows, feature = tokens.shape
    width = w_gate.shape[2]
    wid, _ = unit_columns(feature)
    rows = NZ * CAP
    wide_piece = wid[WIDE] // SPLIT

    def per_unit(shape, divisor):
        return [pltpu.VMEM((*shape, w // divisor), BF16) for w in wid]

    whole = pl.BlockSpec(memory_space=pltpu.VMEM)
    anywhere = pl.BlockSpec(memory_space=pl.ANY)
    dma = pltpu.SemaphoreType.DMA
    return pl.pallas_call(
        moe_kernel,
        out_shape=jax.ShapeDtypeStruct((tok_rows, feature), BF16),
        in_specs=[anywhere] * 6,
        out_specs=whole,
        scratch_shapes=[
            pltpu.VMEM((tok_rows, feature), BF16),
            pltpu.VMEM((TOP, tok_rows), jnp.int32),
            pltpu.VMEM((TOP, tok_rows), jnp.int32),
            per_unit((NX, HALVES, CAP * SPLIT), SPLIT),
            per_unit((NX, NZ, CAP * SPLIT), SPLIT),
            pltpu.VMEM((NX, 2 * NY, rows, feature), BF16),
            pltpu.VMEM((feature, width), BF16),
            pltpu.VMEM((feature, width), BF16),
            pltpu.VMEM((width, feature), BF16),
            pltpu.VMEM((2 * NY * rows, width), BF16),
            pltpu.VMEM((NX, 2 * NY, rows, feature), BF16),
            pltpu.VMEM((NX, NY, rows, feature), BF16),
            per_unit((NX, rows), 2),
            per_unit((NX, rows), 2),
            pltpu.VMEM((NX, rows, feature), BF16),
            pltpu.VMEM((NX, rows, feature), BF16),
            per_unit((NX, NZ, CAP * SPLIT), SPLIT),
            per_unit((NX, NZ, CAP * SPLIT), SPLIT),
            pltpu.VMEM((HALVES, NY, CAP * SPLIT, wide_piece), BF16),
            pltpu.VMEM((NZ, NY, CAP * SPLIT, wide_piece), BF16),
            pltpu.VMEM((NZ, NY, CAP * SPLIT, wide_piece), BF16),
            pltpu.VMEM((NZ, NY, CAP * SPLIT, wide_piece), BF16),
            pltpu.VMEM((NY, HALVES, CAP * SPLIT, wide_piece), BF16),
            pltpu.VMEM((NY - 1, HALVES, CAP * SPLIT, wide_piece), BF16),
            pltpu.VMEM((2, rows * SPLIT, rows * SPLIT), BF16),
            pltpu.VMEM((NX, SPLIT * tok_rows, HALVES * CAP * SPLIT), F32),
            [pltpu.VMEM((SPLIT * tok_rows, w // SPLIT), F32) for w in wid],
            dma((6,)),
            dma((NC, NX, NZ)),
            dma((NC, NX, NZ)),
            dma((NC, NX, 8)),
            dma((NC, NX, 8)),
            dma((NC, NX, 10)),
            dma((NC, NX, 10)),
            dma((NC, NX, NZ)),
            dma((NC, NX, NZ)),
            dma((2, NY - 1)),
            dma((2, NY - 1)),
        ],
        compiler_params=pltpu.CompilerParams(
            collective_id=0, has_side_effects=True, vmem_limit_bytes=64 * 1024 * 1024 - 65536
        ),
        name="moe",
    )(tokens, expert_ids.T, gate_quota.T, w_gate, w_up, w_down)


def solution(mesh):
    return jax.shard_map(
        on_device,
        mesh=mesh,
        in_specs=(
            P(("dp", "expert"), None),
            P(("dp", "expert"), None),
            P(("dp", "expert"), None),
            P("expert", None, "dp"),
            P("expert", None, "dp"),
            P("expert", "dp", None),
        ),
        out_specs=P(("dp", "expert"), None),
        check_vma=False,
    )
```

```python
import jax
import jax.numpy as jnp
from jax import lax
from jax.experimental import pallas as pl
from jax.experimental.pallas import tpu as pltpu
from jax.sharding import PartitionSpec as P

MESH = pl.DeviceIdType.MESH
EXPERTS = 8
TOP = 2
CAP = 6
NX = 4
NZ = 8
NY = 4
HALVES = EXPERTS // NX
GROUP = NZ // HALVES
SPLIT = 8
UNITS = (1, 1)
NC = len(UNITS)
WIDE = NC - 1
NCHUNK = NX
WIDE_IN = 1
WIDE_OUT = 1
F32 = jnp.float32
BF16 = jnp.bfloat16
FINAL = (
    (0, 0),
    (0, 1),
    (1, 0),
    (2, 0),
    (3, 0),
    (1, 1),
    (2, 1),
    (3, 1),
)

SEGMENTS = (
    (
        ("rows_0", 0),
        ("rows_1", 0),
        ("rows_0", 1),
        ("forward_0", 0),
        ("rows_0", 2),
        ("far_0", 0),
        ("forward_1", 0),
        ("forward_0", 1),
        ("rows_1", 2),
        ("far_1", 0),
        ("forward_0", 2),
        ("rows_0", 3),
    ),
    (
        ("far_0", 1),
        ("ring_0", 0),
        ("rows_1", 3),
        ("last_0", 0),
        ("rows_wide", 1),
        ("forward_1", 2),
        ("far_0", 2),
        ("ring_1", 0),
    ),
    (
        ("forward_0", 3),
        ("back_0", 0),
        ("last_1", 0),
        ("forward_1", 3),
        ("ring_wide", 1),
        ("far_1", 2),
        ("ring_0", 1),
    ),
    (
        ("back_1", 0),
        ("far_0", 3),
        ("ring_0", 2),
        ("far_1", 3),
        ("last_0", 1),
    ),
    (
        ("last_0", 2),
        ("ring_0", 3),
        ("ring_1", 2),
        ("back_0", 1),
        ("last_0", 3),
        ("last_1", 2),
        ("back_0", 2),
        ("ring_1", 3),
        ("back_0", 3),
        ("back_wide", 1),
        ("back_1", 2),
        ("last_1", 3),
        ("back_1", 3),
    ),
)


def unit_columns(feature):
    wid = [feature * u // sum(UNITS) for u in UNITS]
    return wid, [sum(wid[:c]) for c in range(NC)]


def moe_kernel(
    tok_hbm, ids_hbm, quota_hbm, wg_hbm, wu_hbm, wd_hbm, out_ref,
    tok_ref, ids_ref, quota_ref, packed, arr, xall, wg, wu, wd, hid, part, fromcore, ringa, ringb, lasta, lastb, outgo, ret,
    spread, arr_wide, out_wide, ret_wide, fin, fin_in, perm, mix, acc, w_sem, dsend, drecv, gsend, grecv, rsend, rrecv, bsend, brecv, ysend, yrecv,
):
    tok, feature = tok_ref.shape
    wid, off = unit_columns(feature)
    rows = NZ * CAP
    slots = EXPERTS * CAP
    dp = lax.axis_index("dp")
    ex = lax.axis_index("expert")
    core = lax.rem(dp, 2)
    y = dp // 2
    xx = ex // NZ
    zz = lax.rem(ex, NZ)
    n_ex = NX * NZ
    y_up, y_down, y_far = lax.rem(y + 1, NY), lax.rem(y + NY - 1, NY), lax.rem(y + 2, NY)
    up = y_up * 2 + core
    down = y_down * 2 + core
    far = y_far * 2 + core
    other = y * 2 + (1 - core)

    def both(c):
        return pl.ds(off[c], wid[c])

    def lo(c):
        return pl.ds(off[c], wid[c] // 2)

    def hi(c):
        return pl.ds(off[c] + wid[c] // 2, wid[c] // 2)

    def piece_cols(c, o):
        piece = wid[c] // SPLIT
        return slice(off[c] + o * piece, off[c] + (o + 1) * piece)

    barrier = pltpu.get_barrier_semaphore()

    def greet(i, carry):
        pl.semaphore_signal(
            barrier, inc=1, device_id={"expert": lax.rem(ex + i, n_ex)}, device_id_type=MESH
        )
        return carry

    lax.fori_loop(1, n_ex, greet, 0)
    for peer in (up, down, far, other):
        pl.semaphore_signal(barrier, inc=1, device_id={"dp": peer}, device_id_type=MESH)

    first_loads = [
        pltpu.make_async_copy(ids_hbm, ids_ref, w_sem.at[3]),
        pltpu.make_async_copy(quota_hbm, quota_ref, w_sem.at[4]),
        pltpu.make_async_copy(tok_hbm, tok_ref, w_sem.at[5]),
    ]
    for load in first_loads:
        load.start()
    loads = [
        pltpu.make_async_copy(wg_hbm.at[0], wg, w_sem.at[0]),
        pltpu.make_async_copy(wu_hbm.at[0], wu, w_sem.at[1]),
        pltpu.make_async_copy(wd_hbm.at[0], wd, w_sem.at[2]),
    ]
    for load in loads:
        load.start()

    p_row = lax.broadcasted_iota(jnp.int32, (rows * SPLIT, rows * SPLIT), 0)
    p_col = lax.broadcasted_iota(jnp.int32, (rows * SPLIT, rows * SPLIT), 1)
    perm[0] = jnp.where(p_row == (p_col & (SPLIT - 1)) * rows + (p_col >> 3), 1.0, 0.0).astype(BF16)

    for load in first_loads:
        load.wait()

    lanes = SPLIT * tok
    t_row = lax.broadcasted_iota(jnp.int32, (tok, lanes), 0)
    t_col = lax.broadcasted_iota(jnp.int32, (tok, lanes), 1) & (tok - 1)
    eye = lax.broadcasted_iota(jnp.int32, (tok, tok), 0) == lax.broadcasted_iota(
        jnp.int32, (tok, tok), 1
    )

    def as_column(values):
        grid = jnp.where(eye, jnp.broadcast_to(values, (tok, tok)), 0)
        return jnp.broadcast_to(jnp.sum(grid, axis=1, keepdims=True), (tok, lanes))

    ids = [as_column(ids_ref[k : k + 1, :]) for k in range(TOP)]
    quota = [as_column(quota_ref[k : k + 1, :].astype(F32)) for k in range(TOP)]
    place_of, share_of = [], []
    lane_quota = [
        jnp.sum(jnp.where(t_row == t_col, q, 0.0), axis=0, keepdims=True) for q in quota
    ]
    whole_quota = lane_quota[0] + lane_quota[1]
    for k in range(TOP):
        mine = jnp.sum(jnp.where(t_row == t_col, ids[k], 0), axis=0, keepdims=True)
        before = jnp.zeros((tok, lanes), jnp.int32)
        for other_k in range(TOP):
            before = before + jnp.where((ids[other_k] == mine) & (t_row < t_col), 1, 0)
        position = jnp.sum(before, axis=0, keepdims=True)
        ahead = ((mine // HALVES) + NX - xx) & (NX - 1)
        place_of.append((ahead * HALVES + (mine & (HALVES - 1))) * CAP + position)
        share_of.append(lane_quota[k] / whole_quota)
    s_row = lax.broadcasted_iota(jnp.int32, (slots * SPLIT, lanes), 0)
    s_col = lax.broadcasted_iota(jnp.int32, (slots * SPLIT, lanes), 1)
    same_piece = (s_row & (SPLIT - 1)) == (s_col >> (tok.bit_length() - 1))
    hits = [same_piece & ((s_row >> 3) == place_of[k]) for k in range(TOP)]
    pick = (jnp.where(hits[0], 1.0, 0.0) + jnp.where(hits[1], 1.0, 0.0)).astype(BF16)

    for c in range(NC):
        stacked = jnp.concatenate([tok_ref[:, piece_cols(c, o)] for o in range(SPLIT)], axis=0)
        chosen = jnp.dot(pick, stacked, preferred_element_type=F32).astype(BF16)
        packed[c][...] = chosen.reshape(packed[c].shape)
        arr[c][0, pl.ds(zz, 1)] = packed[c][0, pl.ds(zz // GROUP, 1)]

    spread[:, pl.ds(y, 1)] = packed[WIDE][WIDE_IN][:, None]

    pl.semaphore_wait(barrier, n_ex - 1 + 4)

    def to_expert(k, c, dz):
        z_to = lax.rem(zz + dz, NZ)
        x_to = lax.rem(xx + k, NX)
        return pltpu.make_async_remote_copy(
            packed[c].at[k, z_to // GROUP], arr[c].at[k, zz],
            dsend.at[c, k, dz], drecv.at[c, k, zz],
            device_id={"expert": x_to * NZ + z_to}, device_id_type=MESH,
        )

    def to_expert_wide(dz):
        z_to = lax.rem(zz + dz, NZ)
        x_to = lax.rem(xx + WIDE_IN, NX)
        return pltpu.make_async_remote_copy(
            spread.at[z_to // GROUP], arr_wide.at[zz],
            dsend.at[WIDE, WIDE_IN, dz], drecv.at[WIDE, WIDE_IN, zz],
            device_id={"expert": x_to * NZ + z_to}, device_id_type=MESH,
        )

    def expert_arrival_wide(z_from):
        return pltpu.make_async_remote_copy(
            spread.at[0], arr_wide.at[z_from],
            dsend.at[WIDE, WIDE_IN, 0], drecv.at[WIDE, WIDE_IN, z_from],
            device_id={"expert": ex}, device_id_type=MESH,
        )

    def along_y(d):
        peer = lax.rem(y + d, NY) * 2 + core
        return to_dp(
            packed[WIDE].at[WIDE_IN], spread.at[:, y], ysend.at[0, d - 1], yrecv.at[0, d - 1], peer
        )

    def to_owner_wide(dz):
        z_to = lax.rem(zz + dz, NZ)
        x_to = lax.rem(xx + NX - WIDE_OUT, NX)
        return pltpu.make_async_remote_copy(
            out_wide.at[z_to], ret_wide.at[zz],
            bsend.at[WIDE, WIDE_OUT, dz], brecv.at[WIDE, WIDE_OUT, zz],
            device_id={"expert": x_to * NZ + z_to}, device_id_type=MESH,
        )

    def owner_arrival_wide(z_from):
        return pltpu.make_async_remote_copy(
            out_wide.at[0], ret_wide.at[z_from],
            bsend.at[WIDE, WIDE_OUT, 0], brecv.at[WIDE, WIDE_OUT, z_from],
            device_id={"expert": ex}, device_id_type=MESH,
        )

    def home_y(d):
        y_to = lax.rem(y + d, NY)
        return to_dp(
            fin.at[y_to], fin_in.at[d - 1], ysend.at[1, d - 1], yrecv.at[1, d - 1],
            y_to * 2 + core,
        )

    def expert_arrival(k, c, z_from):
        return pltpu.make_async_remote_copy(
            packed[c].at[k, 0], arr[c].at[k, z_from], dsend.at[c, k, 0], drecv.at[c, k, z_from],
            device_id={"expert": ex}, device_id_type=MESH,
        )

    def to_dp(src, dst, send, recv, peer):
        return pltpu.make_async_remote_copy(
            src, dst, send, recv, device_id={"dp": peer}, device_id_type=MESH
        )

    def g_copy(k, c, n):
        block, cols, peer = [
            (dp, both(c), up), (dp, both(c), down), (dp, both(c), other),
            (down, lo(c), up), (up, hi(c), down),
            (down, both(c), other), (up, both(c), other), (far, both(c), other),
        ][n]
        view = xall.at[k, block, :, cols]
        return to_dp(view, view, gsend.at[c, k, n], grecv.at[c, k, n], peer)

    def r_copy(k, c, n):
        send, recv = rsend.at[c, k, n], rrecv.at[c, k, n]
        if n < 4:
            place = [y_far, y_up, y_down, y][n]
            return to_dp(
                part.at[k, place * 2 + (1 - core), :, both(c)],
                fromcore.at[k, place, :, both(c)], send, recv, other,
            )
        src, cols, dst, peer = [
            (far, lo(c), ringa[c].at[k], up),
            (far, hi(c), ringb[c].at[k], down),
            (up, hi(c), lasta.at[k, :, hi(c)], up),
            (down, lo(c), lastb.at[k, :, lo(c)], down),
            (up, lo(c), lasta.at[k, :, lo(c)], up),
            (down, hi(c), lastb.at[k, :, hi(c)], down),
        ][n - 4]
        return to_dp(part.at[k, src, :, cols], dst, send, recv, peer)

    def to_owner(k, c, dz):
        z_to = lax.rem(zz + dz, NZ)
        x_to = lax.rem(xx + NX - k, NX)
        return pltpu.make_async_remote_copy(
            outgo[c].at[k, z_to], ret[c].at[k, zz], bsend.at[c, k, dz], brecv.at[c, k, zz],
            device_id={"expert": x_to * NZ + z_to}, device_id_type=MESH,
        )

    def owner_arrival(k, c, z_from):
        return pltpu.make_async_remote_copy(
            outgo[c].at[k, 0], ret[c].at[k, z_from], bsend.at[c, k, 0], brecv.at[c, k, z_from],
            device_id={"expert": ex}, device_id_type=MESH,
        )

    def each_z(k, action):
        def one(z, inner):
            action(z)
            return inner

        lax.fori_loop(0, NZ, one, 0)

    for d in range(1, NY):
        along_y(d).start()

    def send_all(k, carry):
        for c in range(NC):
            def one(dz):
                @pl.when((k != 0) | (dz != 0))
                def _():
                    to_expert(k, c, dz).start()

            if c != WIDE:
                each_z(k, one)
            else:
                pl.when(k != WIDE_IN)(lambda: each_z(k, one))
        return carry

    lax.fori_loop(0, WIDE_IN + 1, send_all, 0)
    for d in range(1, NY):
        along_y(d).wait_recv()
    each_z(0, lambda dz: to_expert_wide(dz).start())
    lax.fori_loop(WIDE_IN + 1, NCHUNK, send_all, 0)

    perm[1] = jnp.where(p_col == (p_row & (SPLIT - 1)) * rows + (p_row >> 3), 1.0, 0.0).astype(BF16)
    mix_t = jnp.where(hits[0], share_of[0], 0.0) + jnp.where(hits[1], share_of[1], 0.0)
    share = mix_t.shape[0] // NX
    for k in range(NX):
        mix[k] = mix_t[k * share : (k + 1) * share].T


    def stage_rows(k, c):
        def one(z_from):
            @pl.when((k != 0) | (z_from != zz))
            def _():
                expert_arrival(k, c, z_from).wait_recv()

        each_z(k, one)
        flat = arr[c][k].reshape(NZ * CAP * SPLIT, wid[c] // SPLIT)
        sorted_rows = jnp.dot(perm[0], flat, preferred_element_type=F32).astype(BF16)
        for o in range(SPLIT):
            xall[k, dp, :, piece_cols(c, o)] = sorted_rows[o * rows : (o + 1) * rows]
        for n in range(3):
            g_copy(k, c, n).start()

    def stage_rows_wide():
        each_z(0, lambda z_from: expert_arrival_wide(z_from).wait_recv())
        for n, place in ((2, y), (5, y_down), (6, y_up), (7, y_far)):
            flat = arr_wide[:, pl.ds(place, 1)].reshape(NZ * CAP * SPLIT, wid[WIDE] // SPLIT)
            sorted_rows = jnp.dot(perm[0], flat, preferred_element_type=F32).astype(BF16)
            for o in range(SPLIT):
                xall[WIDE_IN, place * 2 + core, :, piece_cols(WIDE, o)] = sorted_rows[
                    o * rows : (o + 1) * rows
                ]
            g_copy(WIDE_IN, WIDE, n).start()

    def stage_forward(k, c):
        g_copy(k, c, 0).wait_recv()
        g_copy(k, c, 3).start()
        g_copy(k, c, 5).start()
        g_copy(k, c, 1).wait_recv()
        g_copy(k, c, 4).start()
        g_copy(k, c, 6).start()

    def stage_far(k, c):
        g_copy(k, c, 3).wait_recv()
        g_copy(k, c, 4).wait_recv()
        g_copy(k, c, 7).start()

    def stage_compute(k):
        for c in range(NC):
            for n in (2, 5, 6, 7):
                g_copy(k, c, n).wait_recv()

        @pl.when(k == 0)
        def _():
            for load in loads:
                load.wait()

        for m in range(2):
            x_in = xall[k, m * NY : (m + 1) * NY].reshape(NY * rows, feature)
            gate = jnp.dot(x_in, wg[...], preferred_element_type=F32)
            up_act = jnp.dot(x_in, wu[...], preferred_element_type=F32)
            hid[m * NY * rows : (m + 1) * NY * rows] = (
                gate * (1.0 / (1.0 + jnp.exp(-gate))) * up_act
            ).astype(BF16)

        wide = min(wid) // 2
        for c in range(NC):
            def down_block(n, carry):
                cols = pl.ds(pl.multiple_of(off[c] + n * wide, wide), wide)
                got = jnp.dot(hid[...], wd[:, cols], preferred_element_type=F32).astype(BF16)
                part[k, :, :, cols] = got.reshape(2 * NY, rows, wide)
                return carry

            lax.fori_loop(0, wid[c] // wide, down_block, 0)
            for n in range(4):
                r_copy(k, c, n).start()

    def join(k, c, place):
        mine = place * 2 + core
        cols = both(c)
        total = part[k, mine, :, cols].astype(F32) + fromcore[k, place, :, cols].astype(F32)
        part[k, mine, :, cols] = total.astype(BF16)

    def stage_ring(k, c):
        r_copy(k, c, 0).wait_recv()
        join(k, c, y_far)
        r_copy(k, c, 4).start()
        r_copy(k, c, 5).start()
        r_copy(k, c, 1).wait_recv()
        join(k, c, y_up)
        r_copy(k, c, 6).start()
        r_copy(k, c, 2).wait_recv()
        join(k, c, y_down)
        r_copy(k, c, 7).start()

    def to_pieces(k, c, place, extra):
        pieces = []
        for o in range(SPLIT):
            cols = piece_cols(c, o)
            total = part[k, place * 2 + core, :, cols].astype(F32)
            for more in [fromcore.at[k, place]] + extra:
                total = total + more[:, cols].astype(F32)
            pieces.append(total.astype(BF16))
        block = jnp.concatenate(pieces, axis=0)
        return jnp.dot(perm[1], block, preferred_element_type=F32).astype(BF16)

    def stage_ring_wide():
        for n, place in ((0, y_far), (1, y_up), (2, y_down), (3, y)):
            r_copy(WIDE_OUT, WIDE, n).wait_recv()
            sorted_rows = to_pieces(WIDE_OUT, WIDE, place, [])
            out_wide[:, pl.ds(place, 1)] = sorted_rows.reshape(
                NZ, 1, CAP * SPLIT, wid[WIDE] // SPLIT
            )
        each_z(0, lambda dz: to_owner_wide(dz).start())

    def stage_back_wide():
        each_z(0, lambda z_from: owner_arrival_wide(z_from).wait_recv())
        for place in range(NY):
            for h in range(HALVES):
                total = ret_wide[h * GROUP, place].astype(F32)
                for g in range(1, GROUP):
                    total = total + ret_wide[h * GROUP + g, place].astype(F32)
                fin[place, h] = total.astype(BF16)
        for d in range(1, NY):
            home_y(d).start()

    def stage_last(k, c):
        r_copy(k, c, 4).wait_recv()
        part[k, up, :, lo(c)] = (
            part[k, up, :, lo(c)].astype(F32) + ringa[c][k].astype(F32)
        ).astype(BF16)
        r_copy(k, c, 8).start()
        r_copy(k, c, 5).wait_recv()
        part[k, down, :, hi(c)] = (
            part[k, down, :, hi(c)].astype(F32) + ringb[c][k].astype(F32)
        ).astype(BF16)
        r_copy(k, c, 9).start()

    def stage_back(k, c):
        r_copy(k, c, 3).wait_recv()
        for n in (6, 7, 8, 9):
            r_copy(k, c, n).wait_recv()
        sorted_rows = to_pieces(k, c, y, [lasta.at[k], lastb.at[k]])
        outgo[c][k] = sorted_rows.reshape(NZ, CAP * SPLIT, wid[c] // SPLIT)

        def one(dz):
            @pl.when((k != 0) | (dz != 0))
            def _():
                to_owner(k, c, dz).start()

        each_z(k, one)

        @pl.when(k == 0)
        def _():
            ret[c][0, pl.ds(zz, 1)] = outgo[c][0, pl.ds(zz, 1)]

    todo = {
        "rows": stage_rows, "forward": stage_forward, "far": stage_far,
        "ring": stage_ring, "last": stage_last, "back": stage_back,
    }

    def run(stage, k):
        name, _, c = stage.partition("_")
        if stage == "rows_wide":
            stage_rows_wide()
        elif stage == "ring_wide":
            stage_ring_wide()
        elif stage == "back_wide":
            stage_back_wide()
        else:
            todo[name](k, int(c))

    def step(i, carry):
        for at, segment in enumerate(SEGMENTS):
            @pl.when(i == at)
            def _(segment=segment):
                for stage, k in segment:
                    run(stage, k)

        @pl.when(i < NCHUNK)
        def _():
            stage_compute(i)

        return carry

    lax.fori_loop(0, NCHUNK + 1, step, 0)

    for at, (k, c) in enumerate(FINAL):
        if (c, k) == (WIDE, WIDE_OUT):
            for d in range(1, NY):
                home_y(d).wait_recv()
        else:
            def one(z):
                if k == 0:
                    pl.when(z != zz)(lambda: owner_arrival(k, c, z).wait_recv())
                else:
                    owner_arrival(k, c, z).wait_recv()

            each_z(k, one)
        sums = []
        for h in range(HALVES):
            if (c, k) == (WIDE, WIDE_OUT):
                total = fin[pl.ds(y, 1), h].astype(F32).reshape(fin.shape[2:])
                for d in range(NY - 1):
                    total = total + fin_in[d, h].astype(F32)
            else:
                total = ret[c][k, h * GROUP].astype(F32)
                for g in range(1, GROUP):
                    total = total + ret[c][k, h * GROUP + g].astype(F32)
            sums.append(total)
        mixed = jnp.dot(
            mix[k], jnp.concatenate(sums, axis=0),
            preferred_element_type=F32, precision=lax.Precision.HIGHEST,
        )
        seen = [kk for kk, cc in FINAL[:at] if cc == c]
        if seen:
            mixed = mixed + acc[c][...]
        if len(seen) < NCHUNK - 1:
            acc[c][...] = mixed
        else:
            mixed = mixed.astype(BF16)
            for o in range(SPLIT):
                out_ref[:, piece_cols(c, o)] = mixed[o * tok : (o + 1) * tok]

    def drain(k, carry):
        for c in range(NC):
            def one_in(z):
                @pl.when((k != 0) | (z != 0))
                def _():
                    to_expert(k, c, z).wait_send()

            def one_out(z):
                @pl.when((k != 0) | (z != 0))
                def _():
                    to_owner(k, c, z).wait_send()

            def narrow_in():
                each_z(k, one_in)
                for n in (0, 1, 3, 4):
                    g_copy(k, c, n).wait_send()

            def narrow_out():
                each_z(k, one_out)
                for n in range(4, 10):
                    r_copy(k, c, n).wait_send()

            if c != WIDE:
                narrow_in()
                narrow_out()
            else:
                pl.when(k != WIDE_IN)(narrow_in)
                pl.when(k != WIDE_OUT)(narrow_out)
            for n in (2, 5, 6, 7):
                g_copy(k, c, n).wait_send()
            for n in range(4):
                r_copy(k, c, n).wait_send()
        return carry

    lax.fori_loop(0, NCHUNK, drain, 0)

    def drain_wide(dz):
        to_expert_wide(dz).wait_send()
        to_owner_wide(dz).wait_send()

    each_z(0, drain_wide)
    for d in range(1, NY):
        along_y(d).wait_send()
        home_y(d).wait_send()


def on_device(tokens, expert_ids, gate_quota, w_gate, w_up, w_down):
    tok_rows, feature = tokens.shape
    width = w_gate.shape[2]
    wid, _ = unit_columns(feature)
    rows = NZ * CAP
    wide_piece = wid[WIDE] // SPLIT

    def per_unit(shape, divisor):
        return [pltpu.VMEM((*shape, w // divisor), BF16) for w in wid]

    whole = pl.BlockSpec(memory_space=pltpu.VMEM)
    anywhere = pl.BlockSpec(memory_space=pl.ANY)
    dma = pltpu.SemaphoreType.DMA
    return pl.pallas_call(
        moe_kernel,
        out_shape=jax.ShapeDtypeStruct((tok_rows, feature), BF16),
        in_specs=[anywhere] * 6,
        out_specs=whole,
        scratch_shapes=[
            pltpu.VMEM((tok_rows, feature), BF16),
            pltpu.VMEM((TOP, tok_rows), jnp.int32),
            pltpu.VMEM((TOP, tok_rows), jnp.int32),
            per_unit((NX, HALVES, CAP * SPLIT), SPLIT),
            per_unit((NX, NZ, CAP * SPLIT), SPLIT),
            pltpu.VMEM((NX, 2 * NY, rows, feature), BF16),
            pltpu.VMEM((feature, width), BF16),
            pltpu.VMEM((feature, width), BF16),
            pltpu.VMEM((width, feature), BF16),
            pltpu.VMEM((2 * NY * rows, width), BF16),
            pltpu.VMEM((NX, 2 * NY, rows, feature), BF16),
            pltpu.VMEM((NX, NY, rows, feature), BF16),
            per_unit((NX, rows), 2),
            per_unit((NX, rows), 2),
            pltpu.VMEM((NX, rows, feature), BF16),
            pltpu.VMEM((NX, rows, feature), BF16),
            per_unit((NX, NZ, CAP * SPLIT), SPLIT),
            per_unit((NX, NZ, CAP * SPLIT), SPLIT),
            pltpu.VMEM((HALVES, NY, CAP * SPLIT, wide_piece), BF16),
            pltpu.VMEM((NZ, NY, CAP * SPLIT, wide_piece), BF16),
            pltpu.VMEM((NZ, NY, CAP * SPLIT, wide_piece), BF16),
            pltpu.VMEM((NZ, NY, CAP * SPLIT, wide_piece), BF16),
            pltpu.VMEM((NY, HALVES, CAP * SPLIT, wide_piece), BF16),
            pltpu.VMEM((NY - 1, HALVES, CAP * SPLIT, wide_piece), BF16),
            pltpu.VMEM((2, rows * SPLIT, rows * SPLIT), BF16),
            pltpu.VMEM((NX, SPLIT * tok_rows, HALVES * CAP * SPLIT), F32),
            [pltpu.VMEM((SPLIT * tok_rows, w // SPLIT), F32) for w in wid],
            dma((6,)),
            dma((NC, NX, NZ)),
            dma((NC, NX, NZ)),
            dma((NC, NX, 8)),
            dma((NC, NX, 8)),
            dma((NC, NX, 10)),
            dma((NC, NX, 10)),
            dma((NC, NX, NZ)),
            dma((NC, NX, NZ)),
            dma((2, NY - 1)),
            dma((2, NY - 1)),
        ],
        compiler_params=pltpu.CompilerParams(
            collective_id=0, has_side_effects=True, vmem_limit_bytes=64 * 1024 * 1024 - 65536
        ),
        name="moe",
    )(tokens, expert_ids.T, gate_quota.T, w_gate, w_up, w_down)


def solution(mesh):
    return jax.shard_map(
        on_device,
        mesh=mesh,
        in_specs=(
            P(("dp", "expert"), None),
            P(("dp", "expert"), None),
            P(("dp", "expert"), None),
            P("expert", None, "dp"),
            P("expert", None, "dp"),
            P("expert", "dp", None),
        ),
        out_specs=P(("dp", "expert"), None),
        check_vma=False,
    )
```
